32 devices in a mesh: fsdp: 2 (over x), ctx: 4 (over z), tp: 4 (over y, core).
Axes of the slice: x: 2, y: 2, z: 4, core: 2. Of those that a mesh axis runs over, the one named last changes fastest.
Arguments:
- layer_input: bfloat16 [4096, 2048], P(('fsdp', 'ctx')), may hold values from -6 to 6
- seq_lengths: int32 [2, 3], P('fsdp'), may hold values from 1 to 1536, 2048 in all within a row
- attn_gain: bfloat16 [2048], P('fsdp'), may hold values from 0.25 to 1.75
- query_weight: bfloat16 [2048, 2048], P('fsdp', 'tp'), may hold values from -0.125 to 0.125
- key_matrix: bfloat16 [2048, 1024], P('fsdp', 'tp'), may hold values from -0.125 to 0.125
- value_matrix: bfloat16 [2048, 1024], P('fsdp', 'tp'), may hold values from -0.125 to 0.125
- query_gain: bfloat16 [128], P('fsdp'), may hold values from 0.5 to 5.5
- key_gain: bfloat16 [128], P('fsdp'), may hold values from 0.5 to 5.5
- output_matrix: bfloat16 [2048, 2048], P('tp', 'fsdp'), may hold values from -0.5 to 0.5
- ffn_gain: bfloat16 [2048], P('fsdp'), may hold values from 0.25 to 1.75
- gate_weight: bfloat16 [2048, 6144], P('fsdp', 'tp'), may hold values from -0.125 to 0.125
- up_weight: bfloat16 [2048, 6144], P('fsdp', 'tp'), may hold values from -0.125 to 0.125
- down_weight: bfloat16 [6144, 2048], P('tp', 'fsdp'), may hold values from -0.078125 to 0.078125
- cotangent: bfloat16 [4096, 2048], P(('fsdp', 'ctx')), may hold values from -6 to 6
Outputs:
- layer_output: float32 [4096, 2048], P(('fsdp', 'ctx'))
- input_grad: float32 [4096, 2048], P(('fsdp', 'ctx'))
- attn_gain_grad: float32 [2048], P('fsdp')
- query_weight_grad: float32 [2048, 2048], P('fsdp', 'tp')
- key_weight_grad: float32 [2048, 1024], P('fsdp', 'tp')
- value_weight_grad: float32 [2048, 1024], P('fsdp', 'tp')
- query_gain_grad: float32 [128], P('fsdp')
- key_gain_grad: float32 [128], P('fsdp')
- output_weight_grad: float32 [2048, 2048], P('tp', 'fsdp')
- ffn_gain_grad: float32 [2048], P('fsdp')
- gate_weight_grad: float32 [2048, 6144], P('fsdp', 'tp')
- up_weight_grad: float32 [2048, 6144], P('fsdp', 'tp')
- down_weight_grad: float32 [6144, 2048], P('tp', 'fsdp')
The draws below stay inside these ranges and needn't reach their ends.
Inputs may be any that keep to these rules, and one draw needn't show every extreme that they name: `seq_lengths`: each row sums to 2048, and its longest sequence has exactly 1536 tokens.
All inputs are finite; a program needn't handle non-finite values.
Results may differ from the reference program's by a relative error of at most 0.024.
The reference program's roundings to bfloat16 on the way count: a program that leaves them out, or rounds other values in their place, can miss the bound.
Values may be sent and summed in bfloat16 or wider, within the bound.
A program may use at most 256 MiB of HBM per device.

```python
import math
import jax
import jax.numpy as jnp
import numpy as np
from jax import lax

MODEL_WIDTH = 2048
QUERY_HEADS = 16
KEY_VALUE_HEADS = 8
HEAD_SIZE = 128
FF = 6144
NSEQ = 3
PACK = 2048
LMAX = 1536
TOKENS = 4096
N_FSDP = 2


def head_gain(key):
    values = jnp.clip(1.0 + 0.15 * jax.random.normal(key, (HEAD_SIZE,), jnp.float32), 0.5, 1.5)
    return values.astype(jnp.bfloat16)


def draw_query_gain(key, part):
    return head_gain(jax.random.fold_in(key, 11))


def draw_key_gain(key, part):
    return head_gain(jax.random.fold_in(key, 12))


def shard_levels(stream_key, shape, cuts, smallest, largest):
    gain = 1.0
    for position, shards_of in cuts:
        steps = jax.random.uniform(jax.random.fold_in(jax.random.fold_in(stream_key, 6), position), (shards_of,), jnp.float32, smallest / len(cuts), largest / len(cuts))
        gain = gain * jnp.repeat(jnp.exp(steps), shape[position] // shards_of).reshape((-1,) + (1,) * (len(shape) - 1 - position))
    return gain


def split_up(number_of, total, limit, skew):
    portions = [(1 << 20) // math.isqrt(standing ** skew) + 1 for standing in range(2, number_of + 1)]
    spare, counts = total - limit - (number_of - 1), [1] * (number_of - 1)
    while spare > 0:
        free = [i for i in range(number_of - 1) if counts[i] < limit]
        whole, left = sum([portions[i] for i in free]), spare
        for i in free:
            extra = min(limit - counts[i], max(1, left * portions[i] // whole), spare)
            counts[i] = counts[i] + extra
            spare = spare - extra
    return np.array([limit] + counts)


def uneven(own_key, number_of, total, bound, skew):
    if number_of == 2:
        one = jax.random.randint(own_key, (), max(1, total - bound), min(bound, total - 1) + 1)
        return jnp.stack([one, total - one])
    lengths = jnp.asarray(split_up(number_of, total, bound, skew), jnp.int32)
    couples = (number_of - 1) // 2
    source_of, sink = lengths[1:1 + 2 * couples:2], lengths[2:2 + 2 * couples:2]
    margin = jnp.minimum(source_of - 1, bound - sink)
    passed = jax.random.randint(jax.random.fold_in(own_key, 1), (couples,), 0, 1 << 20) % (margin + 1)
    lengths = lengths.at[1:1 + 2 * couples:2].set(source_of - passed).at[2:2 + 2 * couples:2].set(sink + passed)
    return lengths[jax.random.permutation(jax.random.fold_in(own_key, 2), number_of)]


def normal_values(own_key, extent, spread, reach, shards=(), kind=jnp.bfloat16):
    level = shard_levels(own_key, extent, shards, -0.22, 0.18) if shards else 1.0
    values = jax.random.normal(own_key, extent, jnp.float32) * spread * level
    return jnp.minimum(jnp.maximum(values, -reach), reach).astype(kind)


def setup_inputs(seed: int = 0) -> dict:
    seeds = jax.random.split(jax.random.key(seed), 15)
    layer_input = normal_values(seeds[0], (TOKENS, MODEL_WIDTH), 1.0, 6.0, ((0, 8),))
    seq_lengths = jax.vmap(lambda own: uneven(own, NSEQ, PACK, LMAX, 2))(jax.random.split(seeds[1], N_FSDP)).reshape((N_FSDP, NSEQ)).astype(jnp.int32)
    attn_gain = jnp.clip(1.0 + 0.15 * jax.random.normal(seeds[2], (MODEL_WIDTH,), jnp.float32), 0.25, 1.75).astype(jnp.bfloat16)
    query_weight = normal_values(seeds[3], (MODEL_WIDTH, QUERY_HEADS * HEAD_SIZE), MODEL_WIDTH ** -0.5, 0.125, ((0, 2), (1, 4)))
    key_matrix = normal_values(seeds[4], (MODEL_WIDTH, KEY_VALUE_HEADS * HEAD_SIZE), MODEL_WIDTH ** -0.5, 0.125, ((0, 2), (1, 4)))
    value_matrix = normal_values(seeds[5], (MODEL_WIDTH, KEY_VALUE_HEADS * HEAD_SIZE), MODEL_WIDTH ** -0.5, 0.125, ((0, 2), (1, 4)))
    query_gain = draw_query_gain(jax.random.fold_in(seeds[14], 71), 0)
    key_gain = draw_key_gain(jax.random.fold_in(seeds[14], 71), 0)
    output_matrix = normal_values(seeds[8], (QUERY_HEADS * HEAD_SIZE, MODEL_WIDTH), (QUERY_HEADS * HEAD_SIZE // 16) ** -0.5, 0.5, ((0, 4), (1, 2)))
    ffn_gain = jnp.clip(1.0 + 0.15 * jax.random.normal(seeds[9], (MODEL_WIDTH,), jnp.float32), 0.25, 1.75).astype(jnp.bfloat16)
    gate_weight = normal_values(seeds[10], (MODEL_WIDTH, FF), MODEL_WIDTH ** -0.5, 0.125, ((0, 2), (1, 4)))
    up_weight = normal_values(seeds[11], (MODEL_WIDTH, FF), MODEL_WIDTH ** -0.5, 0.125, ((0, 2), (1, 4)))
    down_weight = normal_values(seeds[12], (FF, MODEL_WIDTH), FF ** -0.5, 0.078125, ((0, 4), (1, 2)))
    cotangent = normal_values(seeds[13], (TOKENS, MODEL_WIDTH), 1.0, 6.0, ((0, 8),))
    return {"layer_input": layer_input, "seq_lengths": seq_lengths, "attn_gain": attn_gain, "query_weight": query_weight, "key_matrix": key_matrix, "value_matrix": value_matrix, "query_gain": query_gain, "key_gain": key_gain, "output_matrix": output_matrix, "ffn_gain": ffn_gain, "gate_weight": gate_weight, "up_weight": up_weight, "down_weight": down_weight, "cotangent": cotangent}


EPSILON = 1e-06
ROPE_BASE = 1000000.0

def segments(seq_lengths, total_rows):
    seq_lengths = seq_lengths.astype(jnp.int32)
    seq_ends = jnp.cumsum(seq_lengths).astype(jnp.int32)
    starts = (seq_ends - seq_lengths).astype(jnp.int32)
    row_index = jnp.arange(total_rows, dtype=jnp.int32)
    seg_ids = lax.optimization_barrier(jnp.sum((row_index[:, None] >= seq_ends[None, :]).astype(jnp.int32), axis=1)).astype(jnp.int32)
    member = seg_ids[:, None] == jnp.arange(seq_lengths.shape[0], dtype=jnp.int32)[None, :]
    offsets = lax.optimization_barrier(jnp.sum(jnp.where(member, starts[None, :], 0), axis=1)).astype(jnp.int32)
    return (seg_ids, (row_index - offsets).astype(jnp.int32))

def rope_tables(positions, width):
    halfway = width // 2
    exponent = jnp.arange(halfway, dtype=jnp.float32) * (2.0 / width)
    frequency = ROPE_BASE ** (-exponent)
    phase_angle = positions.astype(jnp.float32)[:, None] * frequency[None, :]
    return (jnp.cos(phase_angle)[:, None, :], jnp.sin(phase_angle)[:, None, :])

def apply_rotation(values, cosine_table, sine_values):
    halfway = values.shape[-1] // 2
    front_half = values[..., :halfway]
    back_half = values[..., halfway:]
    return jnp.concatenate([front_half * cosine_table - back_half * sine_values, back_half * cosine_table + front_half * sine_values], axis=-1)

def unrotate(upstream, cosine_table, sine_values):
    halfway = upstream.shape[-1] // 2
    front_half = upstream[..., :halfway]
    back_half = upstream[..., halfway:]
    return jnp.concatenate([front_half * cosine_table + back_half * sine_values, back_half * cosine_table - front_half * sine_values], axis=-1)

def row_norm(raw):
    inverse = lax.rsqrt(lax.optimization_barrier(jnp.mean(raw * raw, axis=-1, keepdims=True)) + EPSILON)
    return (raw * inverse, inverse)

def norm_backward(scaled_upstream, normed, inverse):
    return inverse * (scaled_upstream - normed * lax.optimization_barrier(jnp.mean(scaled_upstream * normed, axis=-1, keepdims=True)))

def outer_sum(left, right):
    return lax.dot_general(left, right, (((0,), (0,)), ((), ())), preferred_element_type=jnp.float32)

def product_backward(left, right):
    return lax.dot_general(left, right, (((1,), (1,)), ((), ())), preferred_element_type=jnp.float32)

def visible_mask(query_rows, query_seg, key_seg):
    key_rows = jnp.arange(key_seg.shape[0], dtype=jnp.int32)
    return (query_seg[:, None] == key_seg[None, :]) & (key_rows[None, :] <= query_rows[:, None])

def score_product(queries, keys):
    return jnp.einsum('bkgd,skd->kgbs', queries.astype(jnp.float32), keys.astype(jnp.float32))

def mix_values(weights, values):
    return jnp.einsum('kgbs,skd->bkgd', weights.astype(jnp.float32), values.astype(jnp.float32))

def back_keys(weights, queries):
    return jnp.einsum('kgbs,bkgd->skd', weights.astype(jnp.float32), queries.astype(jnp.float32))

def block_scores(queries, keys, mask):
    scores = score_product(queries, keys) * queries.shape[-1] ** (-0.5)
    return jnp.where(mask[None, None], scores, -jnp.inf)

def block_mask(seg_ids, row_offset, number, block):
    first_row = row_offset + number * block
    query_rows = first_row + jnp.arange(block, dtype=jnp.int32)
    query_seg = lax.dynamic_slice_in_dim(seg_ids, first_row, block)
    return visible_mask(query_rows, query_seg, seg_ids)

def forward_attention(query_rotated, key_rot, value_lines, seg_ids, block, row_offset):
    token_rows = query_rotated.shape[0]
    count = token_rows // block
    query_blocks = query_rotated.reshape((count, block) + query_rotated.shape[1:])

    def one_block(item):
        queries, number = item
        mask = block_mask(seg_ids, row_offset, number, block)
        scores = block_scores(queries, key_rot, mask)
        peak = lax.optimization_barrier(jnp.max(scores, axis=-1, keepdims=True))
        log_total = peak + jnp.log(lax.optimization_barrier(jnp.sum(jnp.exp(scores - peak), axis=-1, keepdims=True)))
        weights = jnp.exp(scores - log_total).astype(jnp.bfloat16)
        mixed = mix_values(weights, value_lines)
        return (mixed.astype(jnp.bfloat16), log_total[..., 0])
    mixed, log_totals = lax.map(one_block, (query_blocks, jnp.arange(count, dtype=jnp.int32)))
    return (mixed.reshape(query_rotated.shape), log_totals)

def backward_attention(query_rotated, key_rot, value_lines, seg_ids, log_totals, mixed_gradient, block, row_offset):
    token_rows = query_rotated.shape[0]
    count = token_rows // block
    query_blocks = query_rotated.reshape((count, block) + query_rotated.shape[1:])
    d_blocks = mixed_gradient.reshape((count, block) + mixed_gradient.shape[1:])
    zero_keys = jnp.zeros(key_rot.shape, jnp.float32)

    def one_block(carry, item):
        key_sum, value_total = carry
        queries, log_total, d_block, number = item
        mask = block_mask(seg_ids, row_offset, number, block)
        scores = block_scores(queries, key_rot, mask)
        probs = jnp.exp(scores - log_total[..., None])
        d_probs = score_product(d_block, value_lines)
        delta = lax.optimization_barrier(jnp.sum(probs * d_probs, axis=-1, keepdims=True))
        d_scores = (probs * (d_probs - delta) * queries.shape[-1] ** (-0.5)).astype(jnp.bfloat16)
        d_queries = mix_values(d_scores, key_rot)
        key_sum = key_sum + back_keys(d_scores, queries)
        value_total = value_total + back_keys(probs.astype(jnp.bfloat16), d_block)
        return ((key_sum, value_total), d_queries)
    numbers = jnp.arange(count, dtype=jnp.int32)
    (key_sum, value_total), d_queries = lax.scan(one_block, (zero_keys, zero_keys), (query_blocks, log_totals, d_blocks, numbers))
    return (d_queries.reshape(query_rotated.shape), key_sum, value_total)

def pack_layer(weights, layer_in, upstream, seq_lengths):
    attn_gain, query_weight, key_matrix, value_matrix, query_gain, key_gain, output_matrix, ffn_gain, gate_weight, up_weight, down_weight = weights
    token_rows = layer_in.shape[0]
    query_group_size = QUERY_HEADS // KEY_VALUE_HEADS
    block = min(512, token_rows)
    seg_ids, positions = segments(seq_lengths, token_rows)
    cosine_table, sine_values = rope_tables(positions, HEAD_SIZE)
    resid_in = layer_in.astype(jnp.float32)
    normed_in, inverse_in = row_norm(resid_in)
    attention_input = (normed_in * attn_gain.astype(jnp.float32)).astype(jnp.bfloat16)
    query_raw = jnp.dot(attention_input, query_weight, preferred_element_type=jnp.float32).reshape(token_rows, QUERY_HEADS, HEAD_SIZE)
    key_projected = jnp.dot(attention_input, key_matrix, preferred_element_type=jnp.float32).reshape(token_rows, KEY_VALUE_HEADS, HEAD_SIZE)
    value_lines = jnp.dot(attention_input, value_matrix, preferred_element_type=jnp.float32).astype(jnp.bfloat16).reshape(token_rows, KEY_VALUE_HEADS, HEAD_SIZE)
    query_normalized, query_inv = row_norm(query_raw)
    key_normalized, key_inverse_norm = row_norm(key_projected)
    query_gain_complete = query_gain.astype(jnp.float32)
    key_gain_complete = key_gain.astype(jnp.float32)
    query_rotated = apply_rotation(query_normalized * query_gain_complete, cosine_table, sine_values).astype(jnp.bfloat16).reshape(token_rows, KEY_VALUE_HEADS, query_group_size, HEAD_SIZE)
    key_rot = apply_rotation(key_normalized * key_gain_complete, cosine_table, sine_values).astype(jnp.bfloat16)
    mixed, log_totals = forward_attention(query_rotated, key_rot, value_lines, seg_ids, block, 0)
    mixed_flat = mixed.reshape(token_rows, QUERY_HEADS * HEAD_SIZE)
    middle = resid_in + jnp.dot(mixed_flat, output_matrix, preferred_element_type=jnp.float32)
    normed_mid, inverse_mid = row_norm(middle)
    ffn_scale = ffn_gain.astype(jnp.float32)
    ffn_input = (normed_mid * ffn_scale).astype(jnp.bfloat16)
    gate_vals = jnp.dot(ffn_input, gate_weight, preferred_element_type=jnp.float32)
    up_vals = jnp.dot(ffn_input, up_weight, preferred_element_type=jnp.float32)
    sigma = jax.nn.sigmoid(gate_vals)
    hidden = (gate_vals * sigma * up_vals).astype(jnp.bfloat16)
    layer_output = middle + jnp.dot(hidden, down_weight, preferred_element_type=jnp.float32)
    d_output = upstream.astype(jnp.float32)
    down_grad = outer_sum(hidden, upstream)
    d_hidden = product_backward(upstream, down_weight)
    d_up = (d_hidden * gate_vals * sigma).astype(jnp.bfloat16)
    d_gate = (d_hidden * up_vals * sigma * (1.0 + gate_vals * (1.0 - sigma))).astype(jnp.bfloat16)
    gate_grad = outer_sum(ffn_input, d_gate)
    up_grad = outer_sum(ffn_input, d_up)
    d_ffn_in = product_backward(d_gate, gate_weight) + product_backward(d_up, up_weight)
    ffn_gain_grad = lax.optimization_barrier(jnp.sum(d_ffn_in * normed_mid, axis=0))
    d_middle = d_output + norm_backward(d_ffn_in * ffn_scale, normed_mid, inverse_mid)
    middle_gradient_copy = d_middle.astype(jnp.bfloat16)
    out_grad = outer_sum(mixed_flat, middle_gradient_copy)
    mixed_gradient = product_backward(middle_gradient_copy, output_matrix).astype(jnp.bfloat16).reshape(token_rows, KEY_VALUE_HEADS, query_group_size, HEAD_SIZE)
    d_queries, key_sum, value_total = backward_attention(query_rotated, key_rot, value_lines, seg_ids, log_totals, mixed_gradient, block, 0)
    d_query_gained = unrotate(d_queries.reshape(token_rows, QUERY_HEADS, HEAD_SIZE), cosine_table, sine_values)
    key_gained_gradient = unrotate(key_sum, cosine_table, sine_values)
    qgain_grad = lax.optimization_barrier(jnp.sum(d_query_gained * query_normalized, axis=(0, 1)))
    kgain_grad = lax.optimization_barrier(jnp.sum(key_gained_gradient * key_normalized, axis=(0, 1)))
    d_query_raw = norm_backward(d_query_gained * query_gain_complete, query_normalized, query_inv).astype(jnp.bfloat16).reshape(token_rows, QUERY_HEADS * HEAD_SIZE)
    key_unrotated_gradient = norm_backward(key_gained_gradient * key_gain_complete, key_normalized, key_inverse_norm).astype(jnp.bfloat16).reshape(token_rows, KEY_VALUE_HEADS * HEAD_SIZE)
    value_gradient_copy = value_total.astype(jnp.bfloat16).reshape(token_rows, KEY_VALUE_HEADS * HEAD_SIZE)
    query_grad = outer_sum(attention_input, d_query_raw)
    key_grad = outer_sum(attention_input, key_unrotated_gradient)
    value_grad = outer_sum(attention_input, value_gradient_copy)
    d_attn_in = product_backward(d_query_raw, query_weight) + product_backward(key_unrotated_gradient, key_matrix) + product_backward(value_gradient_copy, value_matrix)
    attn_gain_grad = lax.optimization_barrier(jnp.sum(d_attn_in * normed_in, axis=0))
    input_grad = d_middle + norm_backward(d_attn_in * attn_gain.astype(jnp.float32), normed_in, inverse_in)
    grads = (attn_gain_grad, query_grad, key_grad, value_grad, qgain_grad, kgain_grad, out_grad, ffn_gain_grad, gate_grad, up_grad, down_grad)
    return (layer_output, input_grad, grads)

def reference(layer_input, seq_lengths, attn_gain, query_weight, key_matrix, value_matrix, query_gain, key_gain, output_matrix, ffn_gain, gate_weight, up_weight, down_weight, cotangent):
    weights = (attn_gain, query_weight, key_matrix, value_matrix, query_gain, key_gain, output_matrix, ffn_gain, gate_weight, up_weight, down_weight)
    packs_in = layer_input.reshape(N_FSDP, PACK, MODEL_WIDTH)
    packs_up = cotangent.reshape(N_FSDP, PACK, MODEL_WIDTH)
    zero_grads = tuple((jnp.zeros(weight.shape, jnp.float32) for weight in weights))

    def one_pack(totals, item):
        layer_in, upstream, lengths_row = item
        layer_output, input_grad, grads = pack_layer(weights, layer_in, upstream, lengths_row)
        totals = tuple((total + grad for total, grad in zip(totals, grads)))
        return (totals, (layer_output, input_grad))
    totals, (outputs, input_grads) = lax.scan(one_pack, zero_grads, (packs_in, packs_up, seq_lengths))
    return (outputs.reshape(TOKENS, MODEL_WIDTH), input_grads.reshape(TOKENS, MODEL_WIDTH), totals[0], totals[1], totals[2], totals[3], totals[4], totals[5], totals[6], totals[7], totals[8], totals[9], totals[10])
```

```python
import functools
import math

import jax
import jax.numpy as jnp
from jax import lax
from jax.experimental import pallas as pl
from jax.experimental.pallas import tpu as pltpu
from jax.sharding import PartitionSpec as P

HEAD_SIZE = 128
EPSILON = 1e-06
ROPE_BASE = 1000000.0
BF16 = jnp.bfloat16
F32 = jnp.float32


def rope_tables(positions, width):
    halfway = width // 2
    exponent = jnp.arange(halfway, dtype=F32) * (2.0 / width)
    frequency = ROPE_BASE ** (-exponent)
    phase_angle = positions.astype(F32)[:, None] * frequency[None, :]
    return (jnp.cos(phase_angle)[:, None, :], jnp.sin(phase_angle)[:, None, :])


def apply_rotation(values, cosine_table, sine_values):
    halfway = values.shape[-1] // 2
    front_half = values[..., :halfway]
    back_half = values[..., halfway:]
    return jnp.concatenate(
        [
            front_half * cosine_table - back_half * sine_values,
            back_half * cosine_table + front_half * sine_values,
        ],
        axis=-1,
    )


def row_norm(raw):
    inverse = lax.rsqrt(jnp.mean(raw * raw, axis=-1, keepdims=True) + EPSILON)
    return (raw * inverse, inverse)


def norm_backward(scaled_upstream, normed, inverse):
    return inverse * (
        scaled_upstream - normed * jnp.mean(scaled_upstream * normed, axis=-1, keepdims=True)
    )


def dot(left, right, left_dim=1, right_dim=0):
    return lax.dot_general(
        left, right, (((left_dim,), (right_dim,)), ((), ())), preferred_element_type=F32
    )


def shift_fsdp(x, step):
    n = lax.axis_size("fsdp")
    return lax.ppermute(x, "fsdp", [(k, (k + step) % n) for k in range(n)])


def gather_fsdp(x):
    return [x] + [shift_fsdp(x, s) for s in range(1, lax.axis_size("fsdp"))]


def gather_weight(x, axis):
    n, m = lax.axis_size("fsdp"), lax.axis_size("ctx")
    if m % 2:
        return jnp.concatenate(gather_fsdp(x), axis=axis)
    odd = lax.rem(lax.axis_index("ctx"), 2)
    half = x.shape[0] // 2
    mine = lax.dynamic_slice_in_dim(x, odd * half, half, 0)
    shards = [x]
    for step in range(1, n):
        first = shift_fsdp(mine, step)
        second = lax.ppermute(first, "ctx", [(k, k ^ 1) for k in range(m)])
        shards.append(
            jnp.where(
                odd == 0,
                jnp.concatenate([first, second], axis=0),
                jnp.concatenate([second, first], axis=0),
            )
        )
    return jnp.concatenate(shards, axis=axis)


def tp_bits():
    n = lax.axis_size("tp")
    return n.bit_length() - 1


def swap_tp(x, bit):
    n = lax.axis_size("tp")
    return lax.ppermute(x, "tp", [(k, k ^ (1 << bit)) for k in range(n)])


def tp_order():
    order = [0]
    for bit in reversed(range(tp_bits())):
        order = order + [p ^ (1 << bit) for p in order]
    return order


def scatter_tp(x):
    for bit in range(tp_bits()):
        half = x.shape[0] // 2
        arrived = swap_tp(x[half:].astype(BF16), bit)
        x = x[:half] + arrived.astype(F32)
    return x


def collect_tp(x):
    for bit in reversed(range(tp_bits())):
        x = jnp.concatenate([x, swap_tp(x, bit)], axis=0)
    return x


def collect_peers(x):
    n = lax.axis_size("fsdp")
    return [collect_tp(shift_fsdp(x[s - 1], -s)) for s in range(1, n)]


def line_kernel(size, slack, blocks, chunks, n_in, n_out, *refs):
    ins, outs = refs[:n_in], refs[n_in : n_in + n_out]
    own, arrived, whole, stage, load_sem, sum_send, sum_recv, whole_send, whole_recv, out_sem = refs[
        n_in + n_out :
    ]
    me = lax.axis_index("ctx")
    depth = stage.shape[2]
    last = size - 1

    loads = []
    for stream in range(2):
        for source, column, _, _, start, count in blocks:
            span = count * depth
            width = stage.shape[3]
            loads.append(
                pltpu.make_async_copy(
                    ins[source].at[pl.ds(stream * span, span), pl.ds(column, width)],
                    own.at[stream, pl.ds(start * depth, span), :],
                    load_sem.at[len(loads)],
                )
            )
            loads[-1].start()

    barrier = pltpu.get_barrier_semaphore()

    @pl.when(me > 0)
    def _():
        pl.semaphore_signal(
            barrier, inc=1, device_id={"ctx": me - 1}, device_id_type=pl.DeviceIdType.MESH
        )

    @pl.when(me < last)
    def _():
        pl.semaphore_signal(
            barrier, inc=1, device_id={"ctx": me + 1}, device_id_type=pl.DeviceIdType.MESH
        )

    pl.semaphore_wait(barrier, jnp.minimum(me, 1) + jnp.minimum(last - me, 1))

    for load in loads:
        load.wait()

    def span_of(chunk):
        return pl.ds(pl.multiple_of(chunk * depth, depth), depth)

    def onward(stream, chunk):
        return pltpu.make_async_remote_copy(
            src_ref=own.at[stream, span_of(chunk), :],
            dst_ref=arrived.at[stream, span_of(chunk), :],
            send_sem=sum_send.at[stream, chunk],
            recv_sem=sum_recv.at[stream, chunk],
            device_id={"ctx": me + 1 if stream == 0 else me - 1},
            device_id_type=pl.DeviceIdType.MESH,
        )

    def backward(stream, chunk, source):
        return pltpu.make_async_remote_copy(
            src_ref=source.at[stream, span_of(chunk), :],
            dst_ref=whole.at[stream, span_of(chunk), :],
            send_sem=whole_send.at[stream, chunk],
            recv_sem=whole_recv.at[stream, chunk],
            device_id={"ctx": me - 1 if stream == 0 else me + 1},
            device_id_type=pl.DeviceIdType.MESH,
        )

    def written(stream, slot):
        return pltpu.make_async_copy(
            stage.at[stream, slot],
            outs[0].at[pl.ds(0, depth), pl.ds(0, stage.shape[3])],
            out_sem.at[stream, slot],
        )

    def tick(i, carry):
        for stream in range(2):
            place = me if stream == 0 else last - me
            chunk = i - slack * place

            @pl.when((chunk >= 0) & (chunk < chunks))
            def _():
                @pl.when(place > 0)
                def _():
                    onward(stream, chunk).wait_recv()
                    rows = span_of(chunk)
                    own[stream, rows, :] = (
                        own[stream, rows, :].astype(F32) + arrived[stream, rows, :].astype(F32)
                    ).astype(BF16)

                @pl.when(place < last)
                def _():
                    onward(stream, chunk).start()

                @pl.when(place == last)
                def _():
                    backward(stream, chunk, own).start()

        for stream in range(2):
            place = me if stream == 0 else last - me
            chunk = i - slack * (2 * last - place)

            @pl.when((chunk >= 0) & (chunk < chunks))
            def _():
                slot = lax.rem(chunk, 2)
                rows = span_of(chunk)

                @pl.when(place < last)
                def _():
                    backward(stream, chunk, whole).wait_recv()

                @pl.when((place > 0) & (place < last))
                def _():
                    backward(stream, chunk, whole).start()

                @pl.when(chunk >= 2)
                def _():
                    written(stream, slot).wait()

                @pl.when(place < last)
                def _():
                    stage[stream, slot] = whole[stream, rows, :].astype(F32)

                @pl.when(place == last)
                def _():
                    stage[stream, slot] = own[stream, rows, :].astype(F32)

                for _, _, target, column, start, count in blocks:

                    @pl.when((chunk >= start) & (chunk < start + count))
                    def _():
                        row = (stream * count + chunk - start) * depth
                        pltpu.make_async_copy(
                            stage.at[stream, slot],
                            outs[target].at[
                                pl.ds(pl.multiple_of(row, depth), depth),
                                pl.ds(column, stage.shape[3]),
                            ],
                            out_sem.at[stream, slot],
                        ).start()

        return carry

    lax.fori_loop(0, chunks + 2 * slack * last, tick, 0)

    for stream in range(2):
        place = me if stream == 0 else last - me
        for slot in range(2):
            written(stream, slot).wait()

        def drain(chunk, carry):
            @pl.when(place < last)
            def _():
                onward(stream, chunk).wait_send()

            @pl.when(place > 0)
            def _():
                backward(stream, chunk, whole).wait_send()

            return carry

        lax.fori_loop(0, chunks, drain, 0)


def sum_ctx(grads, splits):
    size = lax.axis_size("ctx")
    widths = [w for split in splits for w in split]
    width = math.gcd(*widths)
    depth = math.gcd(128, *[g.shape[0] // 2 for g in grads])
    blocks, shapes, first = [], [], 0
    for source, (grad, split) in enumerate(zip(grads, splits)):
        count = grad.shape[0] // (2 * depth)
        column = 0
        for piece in split:
            for inner in range(0, piece, width):
                blocks.append((source, column, len(shapes), inner, first, count))
                column += width
                first += count
            shapes.append(jax.ShapeDtypeStruct((grad.shape[0], piece), F32))
    chunks = first
    dma = pltpu.SemaphoreType.DMA
    buffer = pltpu.VMEM((2, chunks * depth, width), BF16)
    moved = 2 * sum(g.size for g in grads)
    return pl.pallas_call(
        functools.partial(
            line_kernel, size, 2, tuple(blocks), chunks, len(grads), len(shapes)
        ),
        in_specs=[pl.BlockSpec(memory_space=pl.ANY)] * len(grads),
        out_specs=[pl.BlockSpec(memory_space=pl.ANY)] * len(shapes),
        out_shape=shapes,
        scratch_shapes=[
            buffer,
            buffer,
            buffer,
            pltpu.VMEM((2, 2, depth, width), F32),
            dma((2 * len(blocks),)),
            dma((2, chunks)),
            dma((2, chunks)),
            dma((2, chunks)),
            dma((2, chunks)),
            dma((2, 2)),
        ],
        compiler_params=pltpu.CompilerParams(
            collective_id=0, has_side_effects=True, vmem_limit_bytes=56 << 20
        ),
        cost_estimate=pl.CostEstimate(
            flops=moved, bytes_accessed=3 * moved, transcendentals=0
        ),
        name="line_sum",
    )(*grads)


def visible(qrow_ref, qstart_ref, krow_ref):
    keys = krow_ref[:, 0:1]
    return (keys <= qrow_ref[0:1, :]) & (keys >= qstart_ref[0:1, :])


def attend_kernel(scale, q_ref, k_ref, v_ref, qrow_ref, qstart_ref, krow_ref, o_ref, lse_ref):
    scores = dot(k_ref[...], q_ref[...], 1, 1) * scale
    scores = jnp.where(visible(qrow_ref, qstart_ref, krow_ref), scores, -jnp.inf)
    peak = jnp.max(scores, axis=0, keepdims=True)
    weights = jnp.exp(scores - peak)
    total = jnp.sum(weights, axis=0, keepdims=True)
    weights = (weights * (1.0 / total)).astype(BF16)
    o_ref[...] = dot(weights, v_ref[...], 0, 0).astype(BF16)
    lse_ref[...] = (peak + jnp.log(total))[None]


def attend(queries, key_values, query_rows, query_starts, key_rows, block):
    rows, width = queries.shape
    heads = width // HEAD_SIZE
    pack_rows, both = key_values.shape
    kv = both // (2 * HEAD_SIZE)
    group = heads // kv
    blocks = rows // block
    return pl.pallas_call(
        functools.partial(attend_kernel, HEAD_SIZE ** (-0.5)),
        grid=(heads, blocks),
        in_specs=[
            pl.BlockSpec((block, HEAD_SIZE), lambda h, b: (b, h)),
            pl.BlockSpec((pack_rows, HEAD_SIZE), lambda h, b: (0, h // group)),
            pl.BlockSpec((pack_rows, HEAD_SIZE), lambda h, b: (0, kv + h // group)),
            pl.BlockSpec((1, block), lambda h, b: (0, b)),
            pl.BlockSpec((1, block), lambda h, b: (0, b)),
            pl.BlockSpec((pack_rows, 128), lambda h, b: (0, 0)),
        ],
        out_specs=[
            pl.BlockSpec((block, HEAD_SIZE), lambda h, b: (b, h)),
            pl.BlockSpec((1, 1, block), lambda h, b: (h, 0, b)),
        ],
        out_shape=[
            jax.ShapeDtypeStruct((rows, width), BF16),
            jax.ShapeDtypeStruct((heads, 1, rows), F32),
        ],
        cost_estimate=pl.CostEstimate(
            flops=4 * rows * pack_rows * width,
            bytes_accessed=4 * rows * width + 4 * pack_rows * both,
            transcendentals=rows * pack_rows * heads,
        ),
        name="attend",
    )(queries, key_values, key_values, query_rows, query_starts, key_rows)


def attend_back_kernel(
    scale,
    steps,
    q_ref,
    k_ref,
    v_ref,
    do_ref,
    lse_ref,
    qrow_ref,
    qstart_ref,
    krow_ref,
    dq_ref,
    dk_ref,
    dv_ref,
    dk_sum,
    dv_sum,
):
    step = pl.program_id(1) * pl.num_programs(2) + pl.program_id(2)

    @pl.when(step == 0)
    def _():
        dk_sum[...] = jnp.zeros_like(dk_sum)
        dv_sum[...] = jnp.zeros_like(dv_sum)

    queries, keys, upstream = q_ref[...], k_ref[...], do_ref[...]
    scores = dot(keys, queries, 1, 1) * scale
    probs = jnp.where(
        visible(qrow_ref, qstart_ref, krow_ref), jnp.exp(scores - lse_ref[0]), 0.0
    )
    d_probs = dot(v_ref[...], upstream, 1, 1)
    delta = jnp.sum(probs * d_probs, axis=0, keepdims=True)
    d_scores = (probs * (d_probs - delta) * scale).astype(BF16)
    dq_ref[...] = dot(d_scores, keys, 0, 0)
    dk_sum[...] += dot(d_scores, queries)
    dv_sum[...] += dot(probs.astype(BF16), upstream)

    @pl.when(step == steps - 1)
    def _():
        dk_ref[...] = dk_sum[...].astype(BF16)
        dv_ref[...] = dv_sum[...].astype(BF16)


def attend_back(
    queries, key_values, upstream, lse, query_rows, query_starts, key_rows, block
):
    rows, width = queries.shape
    heads = width // HEAD_SIZE
    pack_rows, both = key_values.shape
    kv = both // (2 * HEAD_SIZE)
    group = heads // kv
    blocks = rows // block
    return pl.pallas_call(
        functools.partial(attend_back_kernel, HEAD_SIZE ** (-0.5), group * blocks),
        grid=(kv, group, blocks),
        in_specs=[
            pl.BlockSpec((block, HEAD_SIZE), lambda k, g, b: (b, k * group + g)),
            pl.BlockSpec((pack_rows, HEAD_SIZE), lambda k, g, b: (0, k)),
            pl.BlockSpec((pack_rows, HEAD_SIZE), lambda k, g, b: (0, kv + k)),
            pl.BlockSpec((block, HEAD_SIZE), lambda k, g, b: (b, k * group + g)),
            pl.BlockSpec((1, 1, block), lambda k, g, b: (k * group + g, 0, b)),
            pl.BlockSpec((1, block), lambda k, g, b: (0, b)),
            pl.BlockSpec((1, block), lambda k, g, b: (0, b)),
            pl.BlockSpec((pack_rows, 128), lambda k, g, b: (0, 0)),
        ],
        out_specs=[
            pl.BlockSpec((block, HEAD_SIZE), lambda k, g, b: (b, k * group + g)),
            pl.BlockSpec((pack_rows, HEAD_SIZE), lambda k, g, b: (0, k)),
            pl.BlockSpec((pack_rows, HEAD_SIZE), lambda k, g, b: (0, k)),
        ],
        out_shape=[
            jax.ShapeDtypeStruct((rows, width), F32),
            jax.ShapeDtypeStruct((pack_rows, kv * HEAD_SIZE), BF16),
            jax.ShapeDtypeStruct((pack_rows, kv * HEAD_SIZE), BF16),
        ],
        scratch_shapes=[
            pltpu.VMEM((pack_rows, HEAD_SIZE), F32),
            pltpu.VMEM((pack_rows, HEAD_SIZE), F32),
        ],
        cost_estimate=pl.CostEstimate(
            flops=10 * rows * pack_rows * width,
            bytes_accessed=8 * rows * width + 6 * pack_rows * both,
            transcendentals=rows * pack_rows * heads,
        ),
        name="attend_back",
    )(queries, key_values, key_values, upstream, lse, query_rows, query_starts, key_rows)


def per_device(
    layer_input,
    seq_lengths,
    attn_gain,
    query_weight,
    key_matrix,
    value_matrix,
    query_gain,
    key_gain,
    output_matrix,
    ffn_gain,
    gate_weight,
    up_weight,
    down_weight,
    cotangent,
):
    rows, width = layer_input.shape
    fsdp, ctx, tp = (lax.axis_size(name) for name in ("fsdp", "ctx", "tp"))
    i, c, t = (lax.axis_index(name) for name in ("fsdp", "ctx", "tp"))
    piece, part = rows // tp, width // fsdp
    pack_rows = rows * ctx
    order = tp_order()
    q_width, kv_width = query_weight.shape[1], key_matrix.shape[1]
    heads, kv = q_width // HEAD_SIZE, kv_width // HEAD_SIZE

    def arrange(x):
        x = jnp.concatenate(
            [lax.dynamic_slice_in_dim(x, (t ^ o) * piece, piece, 0) for o in order], axis=0
        )
        return jnp.concatenate(
            [
                lax.dynamic_slice_in_dim(x, lax.rem(i - s + fsdp, fsdp) * part, part, 1)
                for s in range(fsdp)
            ],
            axis=1,
        )

    def natural_features(x):
        size = x.shape[-1] // fsdp
        return jnp.concatenate(
            [
                lax.dynamic_slice_in_dim(x, lax.rem(i - j + fsdp, fsdp) * size, size, x.ndim - 1)
                for j in range(fsdp)
            ],
            axis=-1,
        )

    place = jnp.array([order.index(o) for o in range(tp)], jnp.int32)

    def restore(x):
        x = jnp.concatenate(
            [lax.dynamic_slice_in_dim(x, place[t ^ k] * piece, piece, 0) for k in range(tp)],
            axis=0,
        )
        return natural_features(x)

    small = gather_fsdp(jnp.concatenate([attn_gain, ffn_gain, query_gain, key_gain]))
    qkv_own = jnp.concatenate([query_weight, key_matrix, value_matrix], axis=1)
    qkv_full = gather_weight(qkv_own, 0)
    output_full = gather_weight(output_matrix, 1)
    gate_full = gather_weight(gate_weight, 0)
    up_full = gather_weight(up_weight, 0)
    down_full = gather_weight(down_weight, 1)

    g_width = query_gain.shape[0]
    attn_scale = jnp.concatenate([v[:part] for v in small]).astype(F32)
    ffn_scale = jnp.concatenate([v[part : 2 * part] for v in small]).astype(F32)
    q_scale = natural_features(
        jnp.concatenate([v[2 * part : 2 * part + g_width] for v in small])
    ).astype(F32)
    k_scale = natural_features(
        jnp.concatenate([v[2 * part + g_width :] for v in small])
    ).astype(F32)

    ends = jnp.cumsum(seq_lengths[0])
    starts = ends - seq_lengths[0]

    def start_of(index):
        inside = (index[:, None] >= starts[None, :]) & (index[:, None] < ends[None, :])
        return jnp.sum(jnp.where(inside, starts[None, :], 0), axis=1)

    local = jnp.concatenate(
        [(t ^ o) * piece + jnp.arange(piece, dtype=jnp.int32) for o in order]
    )
    query_index = c * rows + local
    query_start = start_of(query_index)
    key_index = (
        jnp.arange(ctx, dtype=jnp.int32)[:, None] * rows + local[None, :]
    ).reshape(pack_rows)
    cosine_table, sine_values = rope_tables(query_index - query_start, HEAD_SIZE)
    query_rows, query_starts = query_index[None, :], query_start[None, :]
    key_rows = jnp.broadcast_to(key_index[:, None], (pack_rows, 128))

    resid = arrange(layer_input)
    upstream = arrange(cotangent)
    resid_in = resid.astype(F32)
    normed_in, _ = row_norm(resid_in)
    attention_input = (normed_in * attn_scale).astype(BF16)
    qkv = dot(attention_input, qkv_full)
    query_raw = qkv[:, :q_width].reshape(rows, heads, HEAD_SIZE)
    key_raw = qkv[:, q_width : q_width + kv_width].reshape(rows, kv, HEAD_SIZE)
    query_normed, query_inverse = row_norm(query_raw)
    key_normed, key_inverse = row_norm(key_raw)
    query_rotated = (
        apply_rotation(query_normed * q_scale, cosine_table, sine_values)
        .astype(BF16)
        .reshape(rows, q_width)
    )
    key_rotated = (
        apply_rotation(key_normed * k_scale, cosine_table, sine_values)
        .astype(BF16)
        .reshape(rows, kv_width)
    )
    key_value = jnp.concatenate([key_rotated, qkv[:, q_width + kv_width :].astype(BF16)], axis=1)
    key_value_all = lax.all_gather(key_value, "ctx", axis=0, tiled=True)
    block = min(256, rows)
    mixed, lse = attend(
        query_rotated, key_value_all, query_rows, query_starts, key_rows, block
    )

    middle = resid_in[:piece] + scatter_tp(dot(mixed, output_full))
    normed_mid, inverse_mid = row_norm(middle)
    ffn_own = (normed_mid * ffn_scale).astype(BF16)
    ffn_input = collect_tp(ffn_own)
    gate_vals = dot(ffn_input, gate_full)
    up_vals = dot(ffn_input, up_full)
    sigma = jax.nn.sigmoid(gate_vals)
    hidden = (gate_vals * sigma * up_vals).astype(BF16)
    d_hidden = dot(upstream, down_full, 1, 1)
    d_up = (d_hidden * gate_vals * sigma).astype(BF16)
    d_gate = (d_hidden * up_vals * sigma * (1.0 + gate_vals * (1.0 - sigma))).astype(BF16)
    d_ffn = scatter_tp(dot(d_gate, gate_full, 1, 1) + dot(d_up, up_full, 1, 1))

    def blocks_of(own):
        return [own[:piece, s * part : (s + 1) * part] for s in range(1, fsdp)]

    upstream_all = [upstream[:, :part]] + collect_peers(blocks_of(upstream))
    attention_all = [attention_input[:, :part]] + collect_peers(blocks_of(attention_input))
    ffn_all = [ffn_input[:, :part]] + collect_peers(blocks_of(ffn_own))

    def from_peers(x):
        return [x] + [shift_fsdp(x, -s) for s in range(1, fsdp)]

    def outer(left, right):
        return functools.reduce(
            jnp.add, [dot(a, b, 0, 0) for a, b in zip(left, right)]
        )

    down_grad = outer(from_peers(hidden), upstream_all).astype(BF16)
    gate_grad = outer(ffn_all, from_peers(d_gate)).astype(BF16)
    up_grad = outer(ffn_all, from_peers(d_up)).astype(BF16)

    ffn_gain_part = jnp.sum(d_ffn * normed_mid, axis=0)
    d_middle = upstream[:piece].astype(F32) + norm_backward(
        d_ffn * ffn_scale, normed_mid, inverse_mid
    )
    d_middle_own = d_middle.astype(BF16)
    d_middle_b = collect_tp(d_middle_own)
    d_mixed = dot(d_middle_b, output_full, 1, 1).astype(BF16)
    d_queries, d_keys, d_values = attend_back(
        query_rotated, key_value_all, d_mixed, lse, query_rows, query_starts, key_rows, block
    )
    d_key_value = lax.psum_scatter(
        jnp.concatenate([d_keys, d_values], axis=1), "ctx", scatter_dimension=0, tiled=True
    )

    middle_all = [d_middle_b[:, :part]] + collect_peers(blocks_of(d_middle_own))
    out_grad = outer(from_peers(mixed), middle_all).astype(BF16)

    branch = scatter_tp(dot(hidden, down_full))
    layer_output = restore(collect_tp((middle + branch).astype(BF16))).astype(F32)

    d_key_rot = d_key_value[:, :kv_width].astype(F32).reshape(rows, kv, HEAD_SIZE)
    d_value_b = d_key_value[:, kv_width:]
    d_query_gained = apply_rotation(
        d_queries.reshape(rows, heads, HEAD_SIZE), cosine_table, -sine_values
    )
    d_key_gained = apply_rotation(d_key_rot, cosine_table, -sine_values)
    qgain_part = jnp.sum(d_query_gained * query_normed, axis=(0, 1))
    kgain_part = jnp.sum(d_key_gained * key_normed, axis=(0, 1))
    d_query_raw = (
        norm_backward(d_query_gained * q_scale, query_normed, query_inverse)
        .astype(BF16)
        .reshape(rows, q_width)
    )
    d_key_raw = (
        norm_backward(d_key_gained * k_scale, key_normed, key_inverse)
        .astype(BF16)
        .reshape(rows, kv_width)
    )
    d_qkv = jnp.concatenate([d_query_raw, d_key_raw, d_value_b], axis=1)
    d_attn_in = scatter_tp(dot(d_qkv, qkv_full, 1, 1))
    qkv_grad = outer(attention_all, from_peers(d_qkv)).astype(BF16)
    normed_own, inverse_own = row_norm(resid_in[:piece])
    attn_gain_part = jnp.sum(d_attn_in * normed_own, axis=0)
    input_grad = d_middle + norm_backward(d_attn_in * attn_scale, normed_own, inverse_own)
    input_grad = restore(collect_tp(input_grad.astype(BF16))).astype(F32)

    vectors = lax.psum(
        jnp.concatenate(
            [
                natural_features(attn_gain_part),
                natural_features(ffn_gain_part),
                qgain_part,
                kgain_part,
            ]
        ),
        ("fsdp", "ctx", "tp"),
    )

    query_grad, key_grad, value_grad, out_grad, gate_grad, up_grad, down_grad = sum_ctx(
        (qkv_grad, out_grad, gate_grad, up_grad, down_grad),
        ((q_width, kv_width, kv_width), (part,), gate_grad.shape[1:], up_grad.shape[1:], (part,)),
    )

    def own(first, size):
        return lax.dynamic_slice_in_dim(vectors, first + i * size, size, 0)

    return (
        layer_output,
        input_grad,
        own(0, part),
        query_grad,
        key_grad,
        value_grad,
        own(2 * width, g_width),
        own(2 * width + HEAD_SIZE, g_width),
        out_grad,
        own(width, part),
        gate_grad,
        up_grad,
        down_grad,
    )


def solution(mesh):
    tokens = P(("fsdp", "ctx"), None)
    vector, wide, tall = P("fsdp"), P("fsdp", "tp"), P("tp", "fsdp")
    return jax.shard_map(
        per_device,
        mesh=mesh,
        in_specs=(
            tokens,
            P("fsdp", None),
            vector,
            wide,
            wide,
            wide,
            vector,
            vector,
            tall,
            vector,
            wide,
            wide,
            tall,
            tokens,
        ),
        out_specs=(
            tokens,
            tokens,
            vector,
            wide,
            wide,
            wide,
            vector,
            vector,
            tall,
            vector,
            wide,
            wide,
            tall,
        ),
        check_vma=False,
    )
```

```python
import functools
import math

import jax
import jax.numpy as jnp
from jax import lax
from jax.experimental import pallas as pl
from jax.experimental.pallas import tpu as pltpu
from jax.sharding import PartitionSpec as P


HEAD_SIZE = 128
EPSILON = 1e-06
ROPE_BASE = 1000000.0
BF16 = jnp.bfloat16
F32 = jnp.float32


def rope_tables(positions, width):
    halfway = width // 2
    exponent = jnp.arange(halfway, dtype=F32) * (2.0 / width)
    frequency = ROPE_BASE ** (-exponent)
    phase_angle = positions.astype(F32)[:, None] * frequency[None, :]
    return (jnp.cos(phase_angle)[:, None, :], jnp.sin(phase_angle)[:, None, :])


def apply_rotation(values, cosine_table, sine_values):
    halfway = values.shape[-1] // 2
    front_half = values[..., :halfway]
    back_half = values[..., halfway:]
    return jnp.concatenate(
        [
            front_half * cosine_table - back_half * sine_values,
            back_half * cosine_table + front_half * sine_values,
        ],
        axis=-1,
    )


def row_norm(raw):
    inverse = lax.rsqrt(jnp.mean(raw * raw, axis=-1, keepdims=True) + EPSILON)
    return (raw * inverse, inverse)


def norm_backward(scaled_upstream, normed, inverse):
    return inverse * (
        scaled_upstream - normed * jnp.mean(scaled_upstream * normed, axis=-1, keepdims=True)
    )


def dot(left, right, left_dim=1, right_dim=0):
    return lax.dot_general(
        left, right, (((left_dim,), (right_dim,)), ((), ())), preferred_element_type=F32
    )


def shift_fsdp(x, step):
    n = lax.axis_size("fsdp")
    return lax.ppermute(x, "fsdp", [(k, (k + step) % n) for k in range(n)])


def gather_fsdp(x):
    return [x] + [shift_fsdp(x, s) for s in range(1, lax.axis_size("fsdp"))]


def gather_weight(x, axis, parts=1):
    n, m = lax.axis_size("fsdp"), lax.axis_size("ctx")
    if m % 2:
        return jnp.concatenate(gather_fsdp(x), axis=axis)
    odd = lax.rem(lax.axis_index("ctx"), 2)
    half = x.shape[0] // 2
    size = half // parts
    shards = [x]
    for step in range(1, n):
        direct, relayed = [], []
        for p in range(parts):
            mine = lax.dynamic_slice_in_dim(x, odd * half + p * size, size, 0)
            direct.append(shift_fsdp(mine, step))
            relayed.append(
                lax.ppermute(direct[-1], "ctx", [(k, k ^ 1) for k in range(m)])
            )
        shards.append(
            jnp.where(
                odd == 0,
                jnp.concatenate(direct + relayed, axis=0),
                jnp.concatenate(relayed + direct, axis=0),
            )
        )
    return jnp.concatenate(shards, axis=axis)


def tp_bits():
    n = lax.axis_size("tp")
    return n.bit_length() - 1


def swap_tp(x, bit):
    n = lax.axis_size("tp")
    return lax.ppermute(x, "tp", [(k, k ^ (1 << bit)) for k in range(n)])


def tp_order():
    order = [0]
    for bit in reversed(range(tp_bits())):
        order = order + [p ^ (1 << bit) for p in order]
    return order


def scatter_tp(x):
    for bit in range(tp_bits()):
        half = x.shape[0] // 2
        arrived = swap_tp(x[half:].astype(BF16), bit)
        x = x[:half] + arrived.astype(F32)
    return x


def collect_tp(x):
    for bit in reversed(range(tp_bits())):
        x = jnp.concatenate([x, swap_tp(x, bit)], axis=0)
    return x


def collect_peers(x):
    n = lax.axis_size("fsdp")
    arrived = [shift_fsdp(x[s - 1], -s) for s in range(1, n)]
    return [collect_tp(v) for v in arrived]


def turn_ctx(x, step):
    n = lax.axis_size("ctx")
    return lax.ppermute(x, "ctx", [(k, (k + step) % n) for k in range(n)])


def line_kernel(size, slack, blocks, chunks, n_in, n_out, *refs):
    ins, outs = refs[:n_in], refs[n_in : n_in + n_out]
    own, arrived, whole, stage, load_sem, sum_send, sum_recv, whole_send, whole_recv, out_sem = refs[
        n_in + n_out :
    ]
    me = lax.axis_index("ctx")
    depth = stage.shape[2]
    last = size - 1

    loads = []
    for stream in range(2):
        for source, column, _, _, start, count in blocks:
            span = count * depth
            width = stage.shape[3]
            loads.append(
                pltpu.make_async_copy(
                    ins[source].at[pl.ds(stream * span, span), pl.ds(column, width)],
                    own.at[stream, pl.ds(start * depth, span), :],
                    load_sem.at[len(loads)],
                )
            )
            loads[-1].start()

    barrier = pltpu.get_barrier_semaphore()

    @pl.when(me > 0)
    def _():
        pl.semaphore_signal(
            barrier, inc=1, device_id={"ctx": me - 1}, device_id_type=pl.DeviceIdType.MESH
        )

    @pl.when(me < last)
    def _():
        pl.semaphore_signal(
            barrier, inc=1, device_id={"ctx": me + 1}, device_id_type=pl.DeviceIdType.MESH
        )

    pl.semaphore_wait(barrier, jnp.minimum(me, 1) + jnp.minimum(last - me, 1))

    for load in loads:
        load.wait()

    def span_of(chunk):
        return pl.ds(pl.multiple_of(chunk * depth, depth), depth)

    def onward(stream, chunk):
        return pltpu.make_async_remote_copy(
            src_ref=own.at[stream, span_of(chunk), :],
            dst_ref=arrived.at[stream, span_of(chunk), :],
            send_sem=sum_send.at[stream, chunk],
            recv_sem=sum_recv.at[stream, chunk],
            device_id={"ctx": me + 1 if stream == 0 else me - 1},
            device_id_type=pl.DeviceIdType.MESH,
        )

    def backward(stream, chunk, source):
        return pltpu.make_async_remote_copy(
            src_ref=source.at[stream, span_of(chunk), :],
            dst_ref=whole.at[stream, span_of(chunk), :],
            send_sem=whole_send.at[stream, chunk],
            recv_sem=whole_recv.at[stream, chunk],
            device_id={"ctx": me - 1 if stream == 0 else me + 1},
            device_id_type=pl.DeviceIdType.MESH,
        )

    def written(stream, slot):
        return pltpu.make_async_copy(
            stage.at[stream, slot],
            outs[0].at[pl.ds(0, depth), pl.ds(0, stage.shape[3])],
            out_sem.at[stream, slot],
        )

    def tick(i, carry):
        for stream in range(2):
            place = me if stream == 0 else last - me
            chunk = i - slack * place

            @pl.when((chunk >= 0) & (chunk < chunks))
            def _():
                @pl.when(place > 0)
                def _():
                    onward(stream, chunk).wait_recv()
                    rows = span_of(chunk)
                    own[stream, rows, :] = (
                        own[stream, rows, :].astype(F32) + arrived[stream, rows, :].astype(F32)
                    ).astype(BF16)

                @pl.when(place < last)
                def _():
                    onward(stream, chunk).start()

                @pl.when(place == last)
                def _():
                    backward(stream, chunk, own).start()

        for stream in range(2):
            place = me if stream == 0 else last - me
            chunk = i - slack * (2 * last - place)

            @pl.when((chunk >= 0) & (chunk < chunks))
            def _():
                slot = lax.rem(chunk, 2)
                rows = span_of(chunk)

                @pl.when(place < last)
                def _():
                    backward(stream, chunk, whole).wait_recv()

                @pl.when((place > 0) & (place < last))
                def _():
                    backward(stream, chunk, whole).start()

                @pl.when(chunk >= 2)
                def _():
                    written(stream, slot).wait()

                @pl.when(place < last)
                def _():
                    stage[stream, slot] = whole[stream, rows, :].astype(F32)

                @pl.when(place == last)
                def _():
                    stage[stream, slot] = own[stream, rows, :].astype(F32)

                for _, _, target, column, start, count in blocks:

                    @pl.when((chunk >= start) & (chunk < start + count))
                    def _():
                        row = (stream * count + chunk - start) * depth
                        pltpu.make_async_copy(
                            stage.at[stream, slot],
                            outs[target].at[
                                pl.ds(pl.multiple_of(row, depth), depth),
                                pl.ds(column, stage.shape[3]),
                            ],
                            out_sem.at[stream, slot],
                        ).start()

        return carry

    lax.fori_loop(0, chunks + 2 * slack * last, tick, 0)

    for stream in range(2):
        place = me if stream == 0 else last - me
        for slot in range(2):
            written(stream, slot).wait()

        def drain(chunk, carry):
            @pl.when(place < last)
            def _():
                onward(stream, chunk).wait_send()

            @pl.when(place > 0)
            def _():
                backward(stream, chunk, whole).wait_send()

            return carry

        lax.fori_loop(0, chunks, drain, 0)


def sum_ctx(grads, splits):
    size = lax.axis_size("ctx")
    widths = [w for split in splits for w in split]
    width = math.gcd(*widths)
    depth = math.gcd(128, *[g.shape[0] // 2 for g in grads])
    blocks, shapes, first = [], [], 0
    for source, (grad, split) in enumerate(zip(grads, splits)):
        count = grad.shape[0] // (2 * depth)
        column = 0
        for piece in split:
            for inner in range(0, piece, width):
                blocks.append((source, column, len(shapes), inner, first, count))
                column += width
                first += count
            shapes.append(jax.ShapeDtypeStruct((grad.shape[0], piece), F32))
    chunks = first
    dma = pltpu.SemaphoreType.DMA
    buffer = pltpu.VMEM((2, chunks * depth, width), BF16)
    moved = 2 * sum(g.size for g in grads)
    return pl.pallas_call(
        functools.partial(
            line_kernel, size, 2, tuple(blocks), chunks, len(grads), len(shapes)
        ),
        in_specs=[pl.BlockSpec(memory_space=pl.ANY)] * len(grads),
        out_specs=[pl.BlockSpec(memory_space=pl.ANY)] * len(shapes),
        out_shape=shapes,
        scratch_shapes=[
            buffer,
            buffer,
            buffer,
            pltpu.VMEM((2, 2, depth, width), F32),
            dma((2 * len(blocks),)),
            dma((2, chunks)),
            dma((2, chunks)),
            dma((2, chunks)),
            dma((2, chunks)),
            dma((2, 2)),
        ],
        compiler_params=pltpu.CompilerParams(
            collective_id=0, has_side_effects=True, vmem_limit_bytes=56 << 20
        ),
        cost_estimate=pl.CostEstimate(
            flops=moved, bytes_accessed=3 * moved, transcendentals=0
        ),
        name="line_sum",
    )(*grads)


def visible(qrow_ref, qstart_ref, krow_ref):
    keys = krow_ref[:, 0:1]
    return (keys <= qrow_ref[0:1, :]) & (keys >= qstart_ref[0:1, :])


def attend_kernel(scale, q_ref, k_ref, v_ref, qrow_ref, qstart_ref, krow_ref, o_ref, lse_ref):
    scores = dot(k_ref[...], q_ref[...], 1, 1) * scale
    scores = jnp.where(visible(qrow_ref, qstart_ref, krow_ref), scores, -jnp.inf)
    peak = jnp.max(scores, axis=0, keepdims=True)
    weights = jnp.exp(scores - peak)
    total = jnp.sum(weights, axis=0, keepdims=True)
    weights = (weights * (1.0 / total)).astype(BF16)
    o_ref[...] = dot(weights, v_ref[...], 0, 0).astype(BF16)
    lse_ref[...] = (peak + jnp.log(total))[None]


def attend(queries, key_values, query_rows, query_starts, key_rows, block):
    rows, width = queries.shape
    heads = width // HEAD_SIZE
    pack_rows, both = key_values.shape
    kv = both // (2 * HEAD_SIZE)
    group = heads // kv
    blocks = rows // block
    return pl.pallas_call(
        functools.partial(attend_kernel, HEAD_SIZE ** (-0.5)),
        grid=(heads, blocks),
        in_specs=[
            pl.BlockSpec((block, HEAD_SIZE), lambda h, b: (b, h)),
            pl.BlockSpec((pack_rows, HEAD_SIZE), lambda h, b: (0, h // group)),
            pl.BlockSpec((pack_rows, HEAD_SIZE), lambda h, b: (0, kv + h // group)),
            pl.BlockSpec((1, block), lambda h, b: (0, b)),
            pl.BlockSpec((1, block), lambda h, b: (0, b)),
            pl.BlockSpec((pack_rows, 128), lambda h, b: (0, 0)),
        ],
        out_specs=[
            pl.BlockSpec((block, HEAD_SIZE), lambda h, b: (b, h)),
            pl.BlockSpec((1, 1, block), lambda h, b: (h, 0, b)),
        ],
        out_shape=[
            jax.ShapeDtypeStruct((rows, width), BF16),
            jax.ShapeDtypeStruct((heads, 1, rows), F32),
        ],
        cost_estimate=pl.CostEstimate(
            flops=4 * rows * pack_rows * width,
            bytes_accessed=4 * rows * width + 4 * pack_rows * both,
            transcendentals=rows * pack_rows * heads,
        ),
        name="attend",
    )(queries, key_values, key_values, query_rows, query_starts, key_rows)


def attend_back_kernel(
    scale,
    steps,
    q_ref,
    k_ref,
    v_ref,
    do_ref,
    lse_ref,
    qrow_ref,
    qstart_ref,
    krow_ref,
    dq_ref,
    dk_ref,
    dv_ref,
    dk_sum,
    dv_sum,
):
    step = pl.program_id(1) * pl.num_programs(2) + pl.program_id(2)

    @pl.when(step == 0)
    def _():
        dk_sum[...] = jnp.zeros_like(dk_sum)
        dv_sum[...] = jnp.zeros_like(dv_sum)

    queries, keys, upstream = q_ref[...], k_ref[...], do_ref[...]
    scores = dot(keys, queries, 1, 1) * scale
    probs = jnp.where(
        visible(qrow_ref, qstart_ref, krow_ref), jnp.exp(scores - lse_ref[0]), 0.0
    )
    d_probs = dot(v_ref[...], upstream, 1, 1)
    delta = jnp.sum(probs * d_probs, axis=0, keepdims=True)
    d_scores = (probs * (d_probs - delta) * scale).astype(BF16)
    dq_ref[...] = dot(d_scores, keys, 0, 0)
    dk_sum[...] += dot(d_scores, queries)
    dv_sum[...] += dot(probs.astype(BF16), upstream)

    @pl.when(step == steps - 1)
    def _():
        dk_ref[...] = dk_sum[...].astype(BF16)
        dv_ref[...] = dv_sum[...].astype(BF16)


def attend_back(
    queries, key_values, upstream, lse, query_rows, query_starts, key_rows, block
):
    rows, width = queries.shape
    heads = width // HEAD_SIZE
    pack_rows, both = key_values.shape
    kv = both // (2 * HEAD_SIZE)
    group = heads // kv
    blocks = rows // block
    return pl.pallas_call(
        functools.partial(attend_back_kernel, HEAD_SIZE ** (-0.5), group * blocks),
        grid=(kv, group, blocks),
        in_specs=[
            pl.BlockSpec((block, HEAD_SIZE), lambda k, g, b: (b, k * group + g)),
            pl.BlockSpec((pack_rows, HEAD_SIZE), lambda k, g, b: (0, k)),
            pl.BlockSpec((pack_rows, HEAD_SIZE), lambda k, g, b: (0, kv + k)),
            pl.BlockSpec((block, HEAD_SIZE), lambda k, g, b: (b, k * group + g)),
            pl.BlockSpec((1, 1, block), lambda k, g, b: (k * group + g, 0, b)),
            pl.BlockSpec((1, block), lambda k, g, b: (0, b)),
            pl.BlockSpec((1, block), lambda k, g, b: (0, b)),
            pl.BlockSpec((pack_rows, 128), lambda k, g, b: (0, 0)),
        ],
        out_specs=[
            pl.BlockSpec((block, HEAD_SIZE), lambda k, g, b: (b, k * group + g)),
            pl.BlockSpec((pack_rows, HEAD_SIZE), lambda k, g, b: (0, k)),
            pl.BlockSpec((pack_rows, HEAD_SIZE), lambda k, g, b: (0, k)),
        ],
        out_shape=[
            jax.ShapeDtypeStruct((rows, width), F32),
            jax.ShapeDtypeStruct((pack_rows, kv * HEAD_SIZE), BF16),
            jax.ShapeDtypeStruct((pack_rows, kv * HEAD_SIZE), BF16),
        ],
        scratch_shapes=[
            pltpu.VMEM((pack_rows, HEAD_SIZE), F32),
            pltpu.VMEM((pack_rows, HEAD_SIZE), F32),
        ],
        cost_estimate=pl.CostEstimate(
            flops=10 * rows * pack_rows * width,
            bytes_accessed=8 * rows * width + 6 * pack_rows * both,
            transcendentals=rows * pack_rows * heads,
        ),
        name="attend_back",
    )(queries, key_values, key_values, upstream, lse, query_rows, query_starts, key_rows)


def per_device(
    layer_input,
    seq_lengths,
    attn_gain,
    query_weight,
    key_matrix,
    value_matrix,
    query_gain,
    key_gain,
    output_matrix,
    ffn_gain,
    gate_weight,
    up_weight,
    down_weight,
    cotangent,
):
    rows, width = layer_input.shape
    fsdp, ctx, tp = (lax.axis_size(name) for name in ("fsdp", "ctx", "tp"))
    i, c, t = (lax.axis_index(name) for name in ("fsdp", "ctx", "tp"))
    piece, part = rows // tp, width // fsdp
    pack_rows = rows * ctx
    order = tp_order()
    q_width, kv_width = query_weight.shape[1], key_matrix.shape[1]
    heads, kv = q_width // HEAD_SIZE, kv_width // HEAD_SIZE

    def arrange(x):
        x = jnp.concatenate(
            [lax.dynamic_slice_in_dim(x, (t ^ o) * piece, piece, 0) for o in order], axis=0
        )
        return jnp.concatenate(
            [
                lax.dynamic_slice_in_dim(x, lax.rem(i - s + fsdp, fsdp) * part, part, 1)
                for s in range(fsdp)
            ],
            axis=1,
        )

    def natural_features(x):
        size = x.shape[-1] // fsdp
        return jnp.concatenate(
            [
                lax.dynamic_slice_in_dim(x, lax.rem(i - j + fsdp, fsdp) * size, size, x.ndim - 1)
                for j in range(fsdp)
            ],
            axis=-1,
        )

    place = jnp.array([order.index(o) for o in range(tp)], jnp.int32)

    def restore(x):
        x = jnp.concatenate(
            [lax.dynamic_slice_in_dim(x, place[t ^ k] * piece, piece, 0) for k in range(tp)],
            axis=0,
        )
        return natural_features(x)

    small = gather_fsdp(jnp.concatenate([attn_gain, ffn_gain, query_gain, key_gain]))
    qkv_own = jnp.concatenate([query_weight, key_matrix, value_matrix], axis=1)
    qkv_full = gather_weight(qkv_own, 0, 2)
    output_full = gather_weight(output_matrix, 1)
    gate_full = gather_weight(gate_weight, 0)
    up_full = gather_weight(up_weight, 0)
    down_full = gather_fsdp(down_weight)
    down_full = jnp.concatenate(down_full, axis=1)

    g_width = query_gain.shape[0]
    attn_scale = jnp.concatenate([v[:part] for v in small]).astype(F32)
    ffn_scale = jnp.concatenate([v[part : 2 * part] for v in small]).astype(F32)
    q_scale = natural_features(
        jnp.concatenate([v[2 * part : 2 * part + g_width] for v in small])
    ).astype(F32)
    k_scale = natural_features(
        jnp.concatenate([v[2 * part + g_width :] for v in small])
    ).astype(F32)

    ends = jnp.cumsum(seq_lengths[0])
    starts = ends - seq_lengths[0]

    def start_of(index):
        inside = (index[:, None] >= starts[None, :]) & (index[:, None] < ends[None, :])
        return jnp.sum(jnp.where(inside, starts[None, :], 0), axis=1)

    local = jnp.concatenate(
        [(t ^ o) * piece + jnp.arange(piece, dtype=jnp.int32) for o in order]
    )
    query_index = c * rows + local
    query_start = start_of(query_index)
    key_index = jnp.concatenate(
        [lax.rem(c - s + ctx, ctx) * rows + local for s in range(ctx)]
    )
    cosine_table, sine_values = rope_tables(query_index - query_start, HEAD_SIZE)
    query_rows, query_starts = query_index[None, :], query_start[None, :]
    key_rows = jnp.broadcast_to(key_index[:, None], (pack_rows, 128))

    resid = arrange(layer_input)
    upstream = arrange(cotangent)
    resid_in = resid.astype(F32)
    normed_in, _ = row_norm(resid_in)
    attention_input = (normed_in * attn_scale).astype(BF16)
    qkv = dot(attention_input, qkv_full)
    query_raw = qkv[:, :q_width].reshape(rows, heads, HEAD_SIZE)
    key_raw = qkv[:, q_width : q_width + kv_width].reshape(rows, kv, HEAD_SIZE)
    query_normed, query_inverse = row_norm(query_raw)
    key_normed, key_inverse = row_norm(key_raw)
    query_rotated = (
        apply_rotation(query_normed * q_scale, cosine_table, sine_values)
        .astype(BF16)
        .reshape(rows, q_width)
    )
    key_rotated = (
        apply_rotation(key_normed * k_scale, cosine_table, sine_values)
        .astype(BF16)
        .reshape(rows, kv_width)
    )
    key_value = jnp.concatenate([key_rotated, qkv[:, q_width + kv_width :].astype(BF16)], axis=1)
    key_value_all = jnp.concatenate(
        [key_value] + [turn_ctx(key_value, s) for s in range(1, ctx)], axis=0
    )
    block = min(256, rows)
    mixed, lse = attend(
        query_rotated, key_value_all, query_rows, query_starts, key_rows, block
    )

    middle = resid_in[:piece] + scatter_tp(dot(mixed, output_full))
    normed_mid, inverse_mid = row_norm(middle)
    ffn_own = (normed_mid * ffn_scale).astype(BF16)
    ffn_input = collect_tp(ffn_own)
    gate_vals = dot(ffn_input, gate_full)
    up_vals = dot(ffn_input, up_full)
    sigma = jax.nn.sigmoid(gate_vals)
    hidden = (gate_vals * sigma * up_vals).astype(BF16)
    d_hidden = dot(upstream, down_full, 1, 1)
    d_up = (d_hidden * gate_vals * sigma).astype(BF16)
    d_gate = (d_hidden * up_vals * sigma * (1.0 + gate_vals * (1.0 - sigma))).astype(BF16)
    d_ffn_part = dot(d_gate, gate_full, 1, 1) + dot(d_up, up_full, 1, 1)
    d_ffn = scatter_tp(d_ffn_part)

    def blocks_of(own):
        return [own[:piece, s * part : (s + 1) * part] for s in range(1, fsdp)]

    upstream_all = [upstream[:, :part]] + collect_peers(blocks_of(upstream))
    attention_all = [attention_input[:, :part]] + collect_peers(blocks_of(attention_input))
    ffn_all = [ffn_input[:, :part]] + collect_peers(blocks_of(ffn_own))

    def from_peers(x):
        return [x] + [shift_fsdp(x, -s) for s in range(1, fsdp)]

    def outer(left, right):
        return functools.reduce(
            jnp.add, [dot(a, b, 0, 0) for a, b in zip(left, right)]
        ).astype(BF16)

    down_grad = outer(from_peers(hidden), upstream_all)
    gate_grad = outer(ffn_all, from_peers(d_gate))
    up_grad = outer(ffn_all, from_peers(d_up))

    ffn_gain_part = jnp.sum(d_ffn * normed_mid, axis=0)
    d_middle = upstream[:piece].astype(F32) + norm_backward(
        d_ffn * ffn_scale, normed_mid, inverse_mid
    )
    d_middle_own = d_middle.astype(BF16)
    d_middle_b = collect_tp(d_middle_own)
    d_mixed = dot(d_middle_b, output_full, 1, 1).astype(BF16)
    d_queries, d_keys, d_values = attend_back(
        query_rotated, key_value_all, d_mixed, lse, query_rows, query_starts, key_rows, block
    )
    hidden_late, d_queries = lax.optimization_barrier((hidden, d_queries))

    def send_home(x):
        parts = [x[:rows]] + [
            turn_ctx(x[s * rows : (s + 1) * rows], -s) for s in range(1, ctx)
        ]
        return functools.reduce(jnp.add, [p.astype(F32) for p in parts])

    d_key_rot = send_home(d_keys).reshape(rows, kv, HEAD_SIZE)
    d_value_b = send_home(d_values).astype(BF16)

    middle_all = [d_middle_b[:, :part]] + collect_peers(blocks_of(d_middle_own))
    out_grad = outer(from_peers(mixed), middle_all)

    branch = scatter_tp(dot(hidden_late, down_full))
    layer_output = restore(collect_tp((middle + branch).astype(BF16))).astype(F32)

    d_query_gained = apply_rotation(
        d_queries.reshape(rows, heads, HEAD_SIZE), cosine_table, -sine_values
    )
    d_key_gained = apply_rotation(d_key_rot, cosine_table, -sine_values)
    qgain_part = jnp.sum(d_query_gained * query_normed, axis=(0, 1))
    kgain_part = jnp.sum(d_key_gained * key_normed, axis=(0, 1))
    d_query_raw = (
        norm_backward(d_query_gained * q_scale, query_normed, query_inverse)
        .astype(BF16)
        .reshape(rows, q_width)
    )
    d_key_raw = (
        norm_backward(d_key_gained * k_scale, key_normed, key_inverse)
        .astype(BF16)
        .reshape(rows, kv_width)
    )
    d_qkv = jnp.concatenate([d_query_raw, d_key_raw, d_value_b], axis=1)
    d_attn_in = scatter_tp(dot(d_qkv, qkv_full, 1, 1))
    qkv_grad = outer(attention_all, from_peers(d_qkv))
    normed_own, inverse_own = row_norm(resid_in[:piece])
    attn_gain_part = jnp.sum(d_attn_in * normed_own, axis=0)
    input_grad = d_middle + norm_backward(d_attn_in * attn_scale, normed_own, inverse_own)
    input_grad = restore(collect_tp(input_grad.astype(BF16))).astype(F32)

    vector = jnp.concatenate(
        [
            natural_features(attn_gain_part),
            natural_features(ffn_gain_part),
            qgain_part,
            kgain_part,
        ]
    )
    for bit in range(tp_bits()):
        vector = vector + swap_tp(vector, bit)
    if fsdp & (fsdp - 1):
        vector = lax.psum(vector, "fsdp")
    else:
        for bit in range(fsdp.bit_length() - 1):
            vector = vector + lax.ppermute(
                vector, "fsdp", [(k, k ^ (1 << bit)) for k in range(fsdp)]
            )
    vector_rows = jnp.zeros((2 * HEAD_SIZE, kv_width), BF16)
    lines = vector.shape[0] // kv_width
    vector_rows = vector_rows.at[:lines].set(
        vector[: lines * kv_width].reshape(lines, kv_width).astype(BF16)
    )
    vector_rows = vector_rows.at[lines, : vector.shape[0] - lines * kv_width].set(
        vector[lines * kv_width :].astype(BF16)
    )

    down_grad, gate_grad, up_grad, out_grad, query_grad, key_grad, value_grad, vectors = sum_ctx(
        (down_grad, gate_grad, up_grad, out_grad, qkv_grad, vector_rows),
        (
            (part,),
            gate_grad.shape[1:],
            up_grad.shape[1:],
            (part,),
            (q_width, kv_width, kv_width),
            (kv_width,),
        ),
    )
    vectors = vectors[: lines + 1].reshape(-1)

    def own(first, size):
        return lax.dynamic_slice_in_dim(vectors, first + i * size, size, 0)

    return (
        layer_output,
        input_grad,
        own(0, part),
        query_grad,
        key_grad,
        value_grad,
        own(2 * width, g_width),
        own(2 * width + HEAD_SIZE, g_width),
        out_grad,
        own(width, part),
        gate_grad,
        up_grad,
        down_grad,
    )


def solution(mesh):
    tokens = P(("fsdp", "ctx"), None)
    vector, wide, tall = P("fsdp"), P("fsdp", "tp"), P("tp", "fsdp")

    return jax.shard_map(
        per_device,
        mesh=mesh,
        in_specs=(
            tokens,
            P("fsdp", None),
            vector,
            wide,
            wide,
            wide,
            vector,
            vector,
            tall,
            vector,
            wide,
            wide,
            tall,
            tokens,
        ),
        out_specs=(
            tokens,
            tokens,
            vector,
            wide,
            wide,
            wide,
            vector,
            vector,
            tall,
            vector,
            wide,
            wide,
            tall,
        ),
        check_vma=False,
    )
```

```python
import functools
import math

import jax
import jax.numpy as jnp
from jax import lax
from jax.experimental import pallas as pl
from jax.experimental.pallas import tpu as pltpu
from jax.sharding import PartitionSpec as P


HEAD_SIZE = 128
EPSILON = 1e-06
ROPE_BASE = 1000000.0
BF16 = jnp.bfloat16
F32 = jnp.float32
FSDP, CTX, TP = "fsdp", "ctx", "tp"


def rope_tables(positions, width):
    halfway = width // 2
    exponent = jnp.arange(halfway, dtype=F32) * (2.0 / width)
    frequency = ROPE_BASE ** (-exponent)
    phase_angle = positions.astype(F32)[:, None] * frequency[None, :]
    return (jnp.cos(phase_angle)[:, None, :], jnp.sin(phase_angle)[:, None, :])


def apply_rotation(values, cosine_table, sine_values):
    halfway = values.shape[-1] // 2
    front_half = values[..., :halfway]
    back_half = values[..., halfway:]
    return jnp.concatenate(
        [
            front_half * cosine_table - back_half * sine_values,
            back_half * cosine_table + front_half * sine_values,
        ],
        axis=-1,
    )


def row_norm(raw):
    inverse = lax.rsqrt(jnp.mean(raw * raw, axis=-1, keepdims=True) + EPSILON)
    return (raw * inverse, inverse)


def norm_backward(scaled_upstream, normed, inverse):
    return inverse * (
        scaled_upstream - normed * jnp.mean(scaled_upstream * normed, axis=-1, keepdims=True)
    )


def dot(left, right, left_dim=1, right_dim=0):
    return lax.dot_general(
        left, right, (((left_dim,), (right_dim,)), ((), ())), preferred_element_type=F32
    )


def shift_fsdp(x, step):
    n = lax.axis_size(FSDP)
    return lax.ppermute(x, FSDP, [(k, (k + step) % n) for k in range(n)])


def gather_fsdp(x):
    return [x] + [shift_fsdp(x, s) for s in range(1, lax.axis_size(FSDP))]


def gather_weight(x, axis, parts=1):
    n, m = lax.axis_size(FSDP), lax.axis_size(CTX)
    if m % 2:
        return jnp.concatenate(gather_fsdp(x), axis=axis)
    odd = lax.rem(lax.axis_index(CTX), 2)
    half = x.shape[0] // 2
    size = half // parts
    shards = [x]
    for step in range(1, n):
        direct, relayed = [], []
        for p in range(parts):
            mine = lax.dynamic_slice_in_dim(x, odd * half + p * size, size, 0)
            direct.append(shift_fsdp(mine, step))
            relayed.append(
                lax.ppermute(direct[-1], CTX, [(k, k ^ 1) for k in range(m)])
            )
        shards.append(
            jnp.where(
                odd == 0,
                jnp.concatenate(direct + relayed, axis=0),
                jnp.concatenate(relayed + direct, axis=0),
            )
        )
    return jnp.concatenate(shards, axis=axis)


def tp_bits():
    n = lax.axis_size(TP)
    return n.bit_length() - 1


def swap_tp(x, bit):
    n = lax.axis_size(TP)
    return lax.ppermute(x, TP, [(k, k ^ (1 << bit)) for k in range(n)])


def tp_order():
    order = [0]
    for bit in reversed(range(tp_bits())):
        order = order + [p ^ (1 << bit) for p in order]
    return order


def scatter_tp(x):
    for bit in range(tp_bits()):
        half = x.shape[0] // 2
        arrived = swap_tp(x[half:].astype(BF16), bit)
        x = x[:half] + arrived.astype(F32)
    return x


def collect_tp(x):
    for bit in reversed(range(tp_bits())):
        arrived = swap_tp(x, bit)
        x = jnp.concatenate([x, arrived], axis=0)
    return x


def collect_tp_direct(x):
    n = lax.axis_size(TP)
    pieces = [x] + [
        lax.ppermute(x, TP, [(k, k ^ o) for k in range(n)]) for o in tp_order()[1:]
    ]
    return jnp.concatenate(pieces, axis=0)


def collect_peers(x):
    n = lax.axis_size(FSDP)
    arrived = [shift_fsdp(x[s - 1], -s) for s in range(1, n)]
    return [collect_tp(v) for v in arrived]


def turn_ctx(x, step):
    n = lax.axis_size(CTX)
    return lax.ppermute(x, CTX, [(k, k + step) for k in range(n) if 0 <= k + step < n])


def line_kernel(size, slack, blocks, chunks, n_in, n_out, *refs):
    ins, outs = refs[:n_in], refs[n_in : n_in + n_out]
    own, arrived, whole, stage, load_sem, sum_send, sum_recv, whole_send, whole_recv, out_sem = refs[
        n_in + n_out :
    ]
    me = lax.axis_index(CTX)
    depth = stage.shape[2]
    last = size - 1

    loads = []
    for stream in range(2):
        for source, column, _, _, start, count in blocks:
            span = count * depth
            width = stage.shape[3]
            loads.append(
                pltpu.make_async_copy(
                    ins[source].at[pl.ds(stream * span, span), pl.ds(column, width)],
                    own.at[stream, pl.ds(start * depth, span), :],
                    load_sem.at[len(loads)],
                )
            )
            loads[-1].start()

    barrier = pltpu.get_barrier_semaphore()

    @pl.when(me > 0)
    def _():
        pl.semaphore_signal(
            barrier, inc=1, device_id={CTX: me - 1}, device_id_type=pl.DeviceIdType.MESH
        )

    @pl.when(me < last)
    def _():
        pl.semaphore_signal(
            barrier, inc=1, device_id={CTX: me + 1}, device_id_type=pl.DeviceIdType.MESH
        )

    pl.semaphore_wait(barrier, jnp.minimum(me, 1) + jnp.minimum(last - me, 1))

    for load in loads:
        load.wait()

    def span_of(chunk):
        return pl.ds(pl.multiple_of(chunk * depth, depth), depth)

    def onward(stream, chunk):
        return pltpu.make_async_remote_copy(
            src_ref=own.at[stream, span_of(chunk), :],
            dst_ref=arrived.at[stream, span_of(chunk), :],
            send_sem=sum_send.at[stream, chunk],
            recv_sem=sum_recv.at[stream, chunk],
            device_id={CTX: me + 1 if stream == 0 else me - 1},
            device_id_type=pl.DeviceIdType.MESH,
        )

    def backward(stream, chunk, source):
        return pltpu.make_async_remote_copy(
            src_ref=source.at[stream, span_of(chunk), :],
            dst_ref=whole.at[stream, span_of(chunk), :],
            send_sem=whole_send.at[stream, chunk],
            recv_sem=whole_recv.at[stream, chunk],
            device_id={CTX: me - 1 if stream == 0 else me + 1},
            device_id_type=pl.DeviceIdType.MESH,
        )

    def written(stream, slot):
        return pltpu.make_async_copy(
            stage.at[stream, slot],
            outs[0].at[pl.ds(0, depth), pl.ds(0, stage.shape[3])],
            out_sem.at[stream, slot],
        )

    def tick(i, carry):
        for stream in range(2):
            place = me if stream == 0 else last - me
            chunk = i - slack * place

            @pl.when((chunk >= 0) & (chunk < chunks))
            def _():
                @pl.when(place > 0)
                def _():
                    onward(stream, chunk).wait_recv()
                    rows = span_of(chunk)
                    own[stream, rows, :] = (
                        own[stream, rows, :].astype(F32) + arrived[stream, rows, :].astype(F32)
                    ).astype(BF16)

                @pl.when(place < last)
                def _():
                    onward(stream, chunk).start()

                @pl.when(place == last)
                def _():
                    backward(stream, chunk, own).start()

        for stream in range(2):
            place = me if stream == 0 else last - me
            chunk = i - slack * (2 * last - place)

            @pl.when((chunk >= 0) & (chunk < chunks))
            def _():
                slot = lax.rem(chunk, 2)
                rows = span_of(chunk)

                @pl.when(place < last)
                def _():
                    backward(stream, chunk, whole).wait_recv()

                @pl.when((place > 0) & (place < last))
                def _():
                    backward(stream, chunk, whole).start()

                @pl.when(chunk >= 2)
                def _():
                    written(stream, slot).wait()

                @pl.when(place < last)
                def _():
                    stage[stream, slot] = whole[stream, rows, :].astype(F32)

                @pl.when(place == last)
                def _():
                    stage[stream, slot] = own[stream, rows, :].astype(F32)

                for _, _, target, column, start, count in blocks:

                    @pl.when((chunk >= start) & (chunk < start + count))
                    def _():
                        row = (stream * count + chunk - start) * depth
                        pltpu.make_async_copy(
                            stage.at[stream, slot],
                            outs[target].at[
                                pl.ds(pl.multiple_of(row, depth), depth),
                                pl.ds(column, stage.shape[3]),
                            ],
                            out_sem.at[stream, slot],
                        ).start()

        return carry

    lax.fori_loop(0, chunks + 2 * slack * last, tick, 0)

    for stream in range(2):
        place = me if stream == 0 else last - me
        for slot in range(2):
            written(stream, slot).wait()

        def drain(chunk, carry):
            @pl.when(place < last)
            def _():
                onward(stream, chunk).wait_send()

            @pl.when(place > 0)
            def _():
                backward(stream, chunk, whole).wait_send()

            return carry

        lax.fori_loop(0, chunks, drain, 0)


def sum_ctx(grads, splits):
    size = lax.axis_size(CTX)
    widths = [w for split in splits for w in split]
    width = math.gcd(*widths)
    depth = math.gcd(128, *[g.shape[0] // 2 for g in grads])
    blocks, shapes, first = [], [], 0
    for source, (grad, split) in enumerate(zip(grads, splits)):
        count = grad.shape[0] // (2 * depth)
        column = 0
        for piece in split:
            for inner in range(0, piece, width):
                blocks.append((source, column, len(shapes), inner, first, count))
                column += width
                first += count
            shapes.append(jax.ShapeDtypeStruct((grad.shape[0], piece), F32))
    chunks = first
    dma = pltpu.SemaphoreType.DMA
    buffer = pltpu.VMEM((2, chunks * depth, width), BF16)
    moved = 2 * sum(g.size for g in grads)
    return pl.pallas_call(
        functools.partial(
            line_kernel, size, 2, tuple(blocks), chunks, len(grads), len(shapes)
        ),
        in_specs=[pl.BlockSpec(memory_space=pl.ANY)] * len(grads),
        out_specs=[pl.BlockSpec(memory_space=pl.ANY)] * len(shapes),
        out_shape=shapes,
        scratch_shapes=[
            buffer,
            buffer,
            buffer,
            pltpu.VMEM((2, 2, depth, width), F32),
            dma((2 * len(blocks),)),
            dma((2, chunks)),
            dma((2, chunks)),
            dma((2, chunks)),
            dma((2, chunks)),
            dma((2, 2)),
        ],
        compiler_params=pltpu.CompilerParams(
            collective_id=0, has_side_effects=True, vmem_limit_bytes=56 << 20
        ),
        cost_estimate=pl.CostEstimate(
            flops=moved, bytes_accessed=3 * moved, transcendentals=0
        ),
        name="lsum",
    )(*grads)


def visible(qrow_ref, qstart_ref, krow_ref):
    keys = krow_ref[:, 0:1]
    return (keys <= qrow_ref[0:1, :]) & (keys >= qstart_ref[0:1, :])


def attend_kernel(scale, q_ref, k_ref, v_ref, qrow_ref, qstart_ref, krow_ref, o_ref, lse_ref):
    scores = dot(k_ref[...], q_ref[...], 1, 1) * scale
    scores = jnp.where(visible(qrow_ref, qstart_ref, krow_ref), scores, -jnp.inf)
    peak = jnp.max(scores, axis=0, keepdims=True)
    weights = jnp.exp(scores - peak)
    total = jnp.sum(weights, axis=0, keepdims=True)
    weights = (weights * (1.0 / total)).astype(BF16)
    o_ref[...] = dot(weights, v_ref[...], 0, 0).astype(BF16)
    lse_ref[...] = (peak + jnp.log(total))[None]


def attend(queries, key_values, query_rows, query_starts, key_rows, block):
    rows, width = queries.shape
    heads = width // HEAD_SIZE
    pack_rows, both = key_values.shape
    kv = both // (2 * HEAD_SIZE)
    group = heads // kv
    blocks = rows // block
    return pl.pallas_call(
        functools.partial(attend_kernel, HEAD_SIZE ** (-0.5)),
        grid=(heads, blocks),
        in_specs=[
            pl.BlockSpec((block, HEAD_SIZE), lambda h, b: (b, h)),
            pl.BlockSpec((pack_rows, HEAD_SIZE), lambda h, b: (0, h // group)),
            pl.BlockSpec((pack_rows, HEAD_SIZE), lambda h, b: (0, kv + h // group)),
            pl.BlockSpec((1, block), lambda h, b: (0, b)),
            pl.BlockSpec((1, block), lambda h, b: (0, b)),
            pl.BlockSpec((pack_rows, 128), lambda h, b: (0, 0)),
        ],
        out_specs=[
            pl.BlockSpec((block, HEAD_SIZE), lambda h, b: (b, h)),
            pl.BlockSpec((1, 1, block), lambda h, b: (h, 0, b)),
        ],
        out_shape=[
            jax.ShapeDtypeStruct((rows, width), BF16),
            jax.ShapeDtypeStruct((heads, 1, rows), F32),
        ],
        cost_estimate=pl.CostEstimate(
            flops=4 * rows * pack_rows * width,
            bytes_accessed=4 * rows * width + 4 * pack_rows * both,
            transcendentals=rows * pack_rows * heads,
        ),
        name="attend",
    )(queries, key_values, key_values, query_rows, query_starts, key_rows)


def attend_back_kernel(
    scale,
    steps,
    q_ref,
    k_ref,
    v_ref,
    do_ref,
    lse_ref,
    qrow_ref,
    qstart_ref,
    krow_ref,
    dq_ref,
    dk_ref,
    dv_ref,
    dk_sum,
    dv_sum,
):
    step = pl.program_id(1) * pl.num_programs(2) + pl.program_id(2)

    @pl.when(step == 0)
    def _():
        dk_sum[...] = jnp.zeros_like(dk_sum)
        dv_sum[...] = jnp.zeros_like(dv_sum)

    queries, keys, upstream = q_ref[...], k_ref[...], do_ref[...]
    scores = dot(keys, queries, 1, 1) * scale
    probs = jnp.where(
        visible(qrow_ref, qstart_ref, krow_ref), jnp.exp(scores - lse_ref[0]), 0.0
    )
    d_probs = dot(v_ref[...], upstream, 1, 1)
    delta = jnp.sum(probs * d_probs, axis=0, keepdims=True)
    d_scores = (probs * (d_probs - delta) * scale).astype(BF16)
    dq_ref[...] = dot(d_scores, keys, 0, 0)
    dk_sum[...] += dot(d_scores, queries)
    dv_sum[...] += dot(probs.astype(BF16), upstream)

    @pl.when(step == steps - 1)
    def _():
        dk_ref[...] = dk_sum[...].astype(BF16)
        dv_ref[...] = dv_sum[...].astype(BF16)


def attend_back(
    queries, key_values, upstream, lse, query_rows, query_starts, key_rows, block
):
    rows, width = queries.shape
    heads = width // HEAD_SIZE
    pack_rows, both = key_values.shape
    kv = both // (2 * HEAD_SIZE)
    group = heads // kv
    blocks = rows // block
    return pl.pallas_call(
        functools.partial(attend_back_kernel, HEAD_SIZE ** (-0.5), group * blocks),
        grid=(kv, group, blocks),
        in_specs=[
            pl.BlockSpec((block, HEAD_SIZE), lambda k, g, b: (b, k * group + g)),
            pl.BlockSpec((pack_rows, HEAD_SIZE), lambda k, g, b: (0, k)),
            pl.BlockSpec((pack_rows, HEAD_SIZE), lambda k, g, b: (0, kv + k)),
            pl.BlockSpec((block, HEAD_SIZE), lambda k, g, b: (b, k * group + g)),
            pl.BlockSpec((1, 1, block), lambda k, g, b: (k * group + g, 0, b)),
            pl.BlockSpec((1, block), lambda k, g, b: (0, b)),
            pl.BlockSpec((1, block), lambda k, g, b: (0, b)),
            pl.BlockSpec((pack_rows, 128), lambda k, g, b: (0, 0)),
        ],
        out_specs=[
            pl.BlockSpec((block, HEAD_SIZE), lambda k, g, b: (b, k * group + g)),
            pl.BlockSpec((pack_rows, HEAD_SIZE), lambda k, g, b: (0, k)),
            pl.BlockSpec((pack_rows, HEAD_SIZE), lambda k, g, b: (0, k)),
        ],
        out_shape=[
            jax.ShapeDtypeStruct((rows, width), F32),
            jax.ShapeDtypeStruct((pack_rows, kv * HEAD_SIZE), BF16),
            jax.ShapeDtypeStruct((pack_rows, kv * HEAD_SIZE), BF16),
        ],
        scratch_shapes=[
            pltpu.VMEM((pack_rows, HEAD_SIZE), F32),
            pltpu.VMEM((pack_rows, HEAD_SIZE), F32),
        ],
        cost_estimate=pl.CostEstimate(
            flops=10 * rows * pack_rows * width,
            bytes_accessed=8 * rows * width + 6 * pack_rows * both,
            transcendentals=rows * pack_rows * heads,
        ),
    )(queries, key_values, key_values, upstream, lse, query_rows, query_starts, key_rows)


def per_device(
    layer_input,
    seq_lengths,
    attn_gain,
    query_weight,
    key_matrix,
    value_matrix,
    query_gain,
    key_gain,
    output_matrix,
    ffn_gain,
    gate_weight,
    up_weight,
    down_weight,
    cotangent,
):
    rows, width = layer_input.shape
    fsdp, ctx, tp = (lax.axis_size(name) for name in (FSDP, CTX, TP))
    i, c, t = (lax.axis_index(name) for name in (FSDP, CTX, TP))
    piece, part = rows // tp, width // fsdp
    pack_rows = rows * ctx
    order = tp_order()
    q_width, kv_width = query_weight.shape[1], key_matrix.shape[1]
    heads, kv = q_width // HEAD_SIZE, kv_width // HEAD_SIZE

    def arrange(x):
        x = jnp.concatenate(
            [lax.dynamic_slice_in_dim(x, (t ^ o) * piece, piece, 0) for o in order], axis=0
        )
        return jnp.concatenate(
            [
                lax.dynamic_slice_in_dim(x, lax.rem(i - s + fsdp, fsdp) * part, part, 1)
                for s in range(fsdp)
            ],
            axis=1,
        )

    def natural_features(x):
        size = x.shape[-1] // fsdp
        return jnp.concatenate(
            [
                lax.dynamic_slice_in_dim(x, lax.rem(i - j + fsdp, fsdp) * size, size, x.ndim - 1)
                for j in range(fsdp)
            ],
            axis=-1,
        )

    place = jnp.array([order.index(o) for o in range(tp)], jnp.int32)

    def restore(x):
        x = jnp.concatenate(
            [lax.dynamic_slice_in_dim(x, place[t ^ k] * piece, piece, 0) for k in range(tp)],
            axis=0,
        )
        return natural_features(x)

    small = gather_fsdp(jnp.concatenate([attn_gain, ffn_gain, query_gain, key_gain]))
    qkv_own = jnp.concatenate([query_weight, key_matrix, value_matrix], axis=1)
    qkv_full = gather_weight(qkv_own, 0, 2)
    output_full = gather_weight(output_matrix, 1)
    gate_full = gather_weight(gate_weight, 0)
    up_full = gather_weight(up_weight, 0)
    down_full = gather_fsdp(down_weight)
    down_full = jnp.concatenate(down_full, axis=1)

    g_width = query_gain.shape[0]
    attn_scale = jnp.concatenate([v[:part] for v in small]).astype(F32)
    ffn_scale = jnp.concatenate([v[part : 2 * part] for v in small]).astype(F32)
    q_scale = natural_features(
        jnp.concatenate([v[2 * part : 2 * part + g_width] for v in small])
    ).astype(F32)
    k_scale = natural_features(
        jnp.concatenate([v[2 * part + g_width :] for v in small])
    ).astype(F32)

    ends = jnp.cumsum(seq_lengths[0])
    starts = ends - seq_lengths[0]

    def start_of(index):
        inside = (index[:, None] >= starts[None, :]) & (index[:, None] < ends[None, :])
        return jnp.sum(jnp.where(inside, starts[None, :], 0), axis=1)

    local = jnp.concatenate(
        [(t ^ o) * piece + jnp.arange(piece, dtype=jnp.int32) for o in order]
    )
    query_index = c * rows + local
    query_start = start_of(query_index)
    key_index = jnp.concatenate(
        [lax.rem(c - s + ctx, ctx) * rows + local for s in range(ctx)]
    )
    cosine_table, sine_values = rope_tables(query_index - query_start, HEAD_SIZE)
    query_rows, query_starts = query_index[None, :], query_start[None, :]
    key_rows = jnp.broadcast_to(key_index[:, None], (pack_rows, 128))

    resid = arrange(layer_input)
    upstream = arrange(cotangent)
    resid_in = resid.astype(F32)
    normed_in, _ = row_norm(resid_in)
    attention_input = (normed_in * attn_scale).astype(BF16)
    qkv = dot(attention_input, qkv_full)
    query_raw = qkv[:, :q_width].reshape(rows, heads, HEAD_SIZE)
    key_raw = qkv[:, q_width : q_width + kv_width].reshape(rows, kv, HEAD_SIZE)
    query_normed, query_inverse = row_norm(query_raw)
    key_normed, key_inverse = row_norm(key_raw)
    query_rotated = (
        apply_rotation(query_normed * q_scale, cosine_table, sine_values)
        .astype(BF16)
        .reshape(rows, q_width)
    )
    key_rotated = (
        apply_rotation(key_normed * k_scale, cosine_table, sine_values)
        .astype(BF16)
        .reshape(rows, kv_width)
    )
    key_value = jnp.concatenate([key_rotated, qkv[:, q_width + kv_width :].astype(BF16)], axis=1)
    key_value_all = jnp.concatenate(
        [key_value] + [turn_ctx(key_value, s) for s in range(1, ctx)], axis=0
    )
    block = min(256, rows)
    mixed, lse = attend(
        query_rotated, key_value_all, query_rows, query_starts, key_rows, block
    )

    middle = resid_in[:piece] + scatter_tp(dot(mixed, output_full))
    normed_mid, inverse_mid = row_norm(middle)
    ffn_own = (normed_mid * ffn_scale).astype(BF16)
    ffn_input = collect_tp(ffn_own)
    gate_vals = dot(ffn_input, gate_full)
    up_vals = dot(ffn_input, up_full)
    sigma = jax.nn.sigmoid(gate_vals)
    hidden = (gate_vals * sigma * up_vals).astype(BF16)
    d_hidden = dot(upstream, down_full, 1, 1)
    d_up = (d_hidden * gate_vals * sigma).astype(BF16)
    d_gate = (d_hidden * up_vals * sigma * (1.0 + gate_vals * (1.0 - sigma))).astype(BF16)
    d_ffn_part = dot(d_gate, gate_full, 1, 1) + dot(d_up, up_full, 1, 1)
    d_ffn = scatter_tp(d_ffn_part)

    def blocks_of(own):
        return [own[:piece, s * part : (s + 1) * part] for s in range(1, fsdp)]

    upstream_all = [upstream[:, :part]] + collect_peers(blocks_of(upstream))
    attention_all = [attention_input[:, :part]] + collect_peers(blocks_of(attention_input))
    ffn_all = [ffn_input[:, :part]] + collect_peers(blocks_of(ffn_own))

    def from_peers(x):
        return [x] + [shift_fsdp(x, -s) for s in range(1, fsdp)]

    def outer(left, right):
        return functools.reduce(
            jnp.add, [dot(a, b, 0, 0) for a, b in zip(left, right)]
        ).astype(BF16)

    down_grad = outer(from_peers(hidden), upstream_all)
    down_sum = lax.psum(down_grad, CTX)
    gate_grad = outer(ffn_all, from_peers(d_gate))
    up_grad = outer(ffn_all, from_peers(d_up))

    ffn_gain_part = jnp.sum(d_ffn * normed_mid, axis=0)
    d_middle = upstream[:piece].astype(F32) + norm_backward(
        d_ffn * ffn_scale, normed_mid, inverse_mid
    )
    d_middle_own = d_middle.astype(BF16)
    d_middle_b = collect_tp(d_middle_own)
    d_mixed = dot(d_middle_b, output_full, 1, 1).astype(BF16)
    d_queries, d_keys, d_values = attend_back(
        query_rotated, key_value_all, d_mixed, lse, query_rows, query_starts, key_rows, block
    )
    hidden_late, d_queries = lax.optimization_barrier((hidden, d_queries))

    def send_home(x):
        parts = [x[:rows]] + [
            turn_ctx(x[s * rows : (s + 1) * rows], -s) for s in range(1, ctx)
        ]
        return functools.reduce(jnp.add, [p.astype(F32) for p in parts])

    d_key_rot = send_home(d_keys).reshape(rows, kv, HEAD_SIZE)
    d_value_b = send_home(d_values).astype(BF16)

    middle_all = [d_middle_b[:, :part]] + collect_peers(blocks_of(d_middle_own))
    out_grad = outer(from_peers(mixed), middle_all)

    branch = scatter_tp(dot(hidden_late, down_full))
    layer_output = restore(collect_tp_direct((middle + branch).astype(BF16))).astype(F32)

    d_query_gained = apply_rotation(
        d_queries.reshape(rows, heads, HEAD_SIZE), cosine_table, -sine_values
    )
    d_key_gained = apply_rotation(d_key_rot, cosine_table, -sine_values)
    qgain_part = jnp.sum(d_query_gained * query_normed, axis=(0, 1))
    kgain_part = jnp.sum(d_key_gained * key_normed, axis=(0, 1))
    d_query_raw = (
        norm_backward(d_query_gained * q_scale, query_normed, query_inverse)
        .astype(BF16)
        .reshape(rows, q_width)
    )
    d_key_raw = (
        norm_backward(d_key_gained * k_scale, key_normed, key_inverse)
        .astype(BF16)
        .reshape(rows, kv_width)
    )
    d_qkv = jnp.concatenate([d_query_raw, d_key_raw, d_value_b], axis=1)
    d_attn_part = dot(d_qkv, qkv_full, 1, 1)
    d_attn_in = scatter_tp(d_attn_part)
    query_grad = outer(attention_all, from_peers(d_query_raw))
    kv_grad = outer(
        attention_all,
        from_peers(jnp.concatenate([d_key_raw, d_value_b], axis=1)),
    )
    normed_own, inverse_own = row_norm(resid_in[:piece])
    attn_gain_part = jnp.sum(d_attn_part * row_norm(resid_in)[0], axis=0)
    input_grad = d_middle + norm_backward(d_attn_in * attn_scale, normed_own, inverse_own)
    input_grad = restore(collect_tp_direct(input_grad.astype(BF16))).astype(F32)

    vector = jnp.concatenate(
        [
            natural_features(attn_gain_part),
            natural_features(ffn_gain_part),
            qgain_part,
            kgain_part,
        ]
    )
    for bit in range(tp_bits()):
        vector = vector + swap_tp(vector, bit)
    if fsdp & (fsdp - 1):
        vector = lax.psum(vector, FSDP)
    else:
        for bit in range(fsdp.bit_length() - 1):
            vector = vector + lax.ppermute(
                vector, FSDP, [(k, k ^ (1 << bit)) for k in range(fsdp)]
            )
    vector_rows = jnp.zeros((2 * HEAD_SIZE, kv_width), BF16)
    lines = vector.shape[0] // kv_width
    vector_rows = vector_rows.at[:lines].set(
        vector[: lines * kv_width].reshape(lines, kv_width).astype(BF16)
    )
    vector_rows = vector_rows.at[lines, : vector.shape[0] - lines * kv_width].set(
        vector[lines * kv_width :].astype(BF16)
    )

    gate_grad, up_grad, out_grad, query_grad, key_grad, value_grad, vectors = sum_ctx(
        (gate_grad, up_grad, out_grad, query_grad, kv_grad, vector_rows),
        (
            gate_grad.shape[1:],
            up_grad.shape[1:],
            (part,),
            (q_width,),
            (kv_width, kv_width),
            (kv_width,),
        ),
    )
    down_sum, vectors = lax.optimization_barrier((down_sum, vectors))
    down_grad = down_sum.astype(F32)
    vectors = vectors[: lines + 1].reshape(-1)

    def own(first, size):
        return lax.dynamic_slice_in_dim(vectors, first + i * size, size, 0)

    return (
        layer_output,
        input_grad,
        own(0, part),
        query_grad,
        key_grad,
        value_grad,
        own(2 * width, g_width),
        own(2 * width + HEAD_SIZE, g_width),
        out_grad,
        own(width, part),
        gate_grad,
        up_grad,
        down_grad,
    )


def solution(mesh):
    tokens = P((FSDP, CTX), None)
    vector, wide, tall = P(FSDP), P(FSDP, TP), P(TP, FSDP)

    return jax.shard_map(
        per_device,
        mesh=mesh,
        in_specs=(
            tokens,
            P(FSDP, None),
            vector,
            wide,
            wide,
            wide,
            vector,
            vector,
            tall,
            vector,
            wide,
            wide,
            tall,
            tokens,
        ),
        out_specs=(
            tokens,
            tokens,
            vector,
            wide,
            wide,
            wide,
            vector,
            vector,
            tall,
            vector,
            wide,
            wide,
            tall,
        ),
        check_vma=False,
    )
```
